512 devices in a mesh: dp: 16 (over z, core), row: 8 (over y), col: 4 (over x).
Axes of the slice: x: 4, y: 8, z: 8, core: 2. Of those that a mesh axis runs over, the one named last changes fastest.
Arguments:
- token_ids: int32 [128, 4], replicated, may hold values from 0 to 81919
- slot_heads: int32 [32], replicated, may hold values from 0 to 31, each once
- embed_table: bfloat16 [81920, 2304], P('dp', ('row', 'col')), may hold values from -6 to 6
- query_weight: bfloat16 [2304, 128, 32], P('col', 'row'), may hold values from -0.125 to 0.125
- key_weight: bfloat16 [2304, 128, 32], P('col', 'row'), may hold values from -0.125 to 0.125
- value_weight: bfloat16 [2304, 128, 32], P('row', 'col'), may hold values from -0.125 to 0.125
- decay_down: bfloat16 [2304, 128], P('col'), may hold values from -0.125 to 0.125
- decay_up: bfloat16 [128, 128, 32], P(None, 'row'), may hold values from -0.5 to 0.5
- decay_bias: float32 [128, 32], P('row'), may hold values from -4 to 4
- decay_rate: float32 [128, 32], P('row'), may hold values from 0.01 to 1.5
- beta_weight: bfloat16 [2304, 32], P('col'), may hold values from -0.125 to 0.125
- init_state: float32 [128, 128, 128, 32], P('dp', 'row', 'col'), may hold values from -80 to 80
Outputs:
- readout: bfloat16 [128, 4, 128, 32], P('dp', None, 'col')
- final_state: float32 [128, 128, 128, 32], P('dp', 'row', 'col')
The draws below stay inside these ranges and needn't reach their ends.
Inputs may be any that keep to these rules, and one draw needn't show every extreme that they name: `slot_heads`: each head once.
All inputs are finite; a program needn't handle non-finite values.
Results may differ from the reference program's by a relative error of at most 0.0022.
Values may be sent and summed in bfloat16 or wider, within the bound.
No kernel may reach another device: no remote copies, remote signals or barrier semaphores. Data moves between devices by JAX's collectives and lax.ppermute only.
A program may use at most 64 MiB of HBM per device.

```python
import math
import jax
import jax.numpy as jnp
from jax import lax

D = 2304
H = 32
DK = 128
DV = 128
R = 128
VOCAB = 81920
STEPS = 4
B = 128


def draw_init_state(key, part):
    keys = jax.random.split(jax.random.fold_in(key, 17), 4)
    head_scale = jnp.exp(jax.random.uniform(keys[0], (B, 1, 1, H), jnp.float32, jnp.log(0.05), jnp.log(0.4)))
    row_ramp = 3.0 ** (jnp.arange(DK, dtype=jnp.float32) / DK)
    col_ramp = 3.0 ** (jnp.arange(DV, dtype=jnp.float32) / DV)
    row_scale = row_ramp[None, :, None, None] * jax.random.uniform(keys[1], (B, DK, 1, H), jnp.float32, 1.0, 1.8)
    col_scale = col_ramp[None, None, :, None] * jax.random.uniform(keys[2], (B, 1, DV, H), jnp.float32, 1.0, 1.8)
    base = jax.random.truncated_normal(keys[3], -6.0, 6.0, (B, DK, DV, H), jnp.float32)
    return (base * head_scale * row_scale * col_scale).astype(jnp.float32)


def with_ends(drawn, own_key, smallest, high):
    index_at = [jax.random.randint(jax.random.fold_in(own_key, axis), (), 0, length) for axis, length in enumerate(drawn.shape)]
    widest = drawn.shape.index(max(drawn.shape))
    next_to = index_at[:widest] + [(index_at[widest] + 1) % drawn.shape[widest]] + index_at[widest + 1:]
    return drawn.at[tuple(index_at)].set(smallest).at[tuple(next_to)].set(high)


def levels(key, dims, cuts, least, top_value):
    def one(axis_at, blocks):
        draws = jax.random.uniform(jax.random.fold_in(jax.random.fold_in(key, 6), axis_at), (blocks,), jnp.float32, least / len(cuts), top_value / len(cuts))
        return jnp.repeat(jnp.exp(draws), dims[axis_at] // blocks).reshape((-1,) + (1,) * (len(dims) - axis_at - 1))

    loudness = one(*cuts[0])
    for cut in cuts[1:]:
        loudness = loudness * one(*cut)
    return loudness


def scatter_about(stream_key, dims, scale, limit, cuts=(), kind=jnp.bfloat16):
    factor_of = levels(stream_key, dims, cuts, -0.22, 0.18) if cuts else 1.0
    entries = jax.random.normal(stream_key, dims, jnp.float32) * scale * factor_of
    return jnp.minimum(jnp.maximum(entries, -limit), limit).astype(kind)


def setup_inputs(seed: int = 0) -> dict:
    seeds = jax.random.split(jax.random.key(seed), 13)
    return {
        "token_ids": with_ends(jax.random.randint(seeds[0], (B, STEPS), 0, VOCAB), jax.random.fold_in(seeds[0], 1), 0, VOCAB - 1).astype(jnp.int32),
        "slot_heads": jax.random.permutation(seeds[1], H).astype(jnp.int32),
        "embed_table": scatter_about(seeds[2], (VOCAB, D), 1.0, 6.0, ((0, 16), (1, 32))),
        "query_weight": scatter_about(seeds[3], (D, DK, H), D ** -0.5, 0.125, ((0, 4), (1, 8))),
        "key_weight": scatter_about(seeds[4], (D, DK, H), D ** -0.5, 0.125, ((0, 4), (1, 8))),
        "value_weight": scatter_about(seeds[5], (D, DV, H), D ** -0.5, 0.125, ((0, 8), (1, 4))),
        "decay_down": scatter_about(seeds[6], (D, R), D ** -0.5, 0.125, ((0, 4),)),
        "decay_up": scatter_about(seeds[7], (R, DK, H), R ** -0.5, 0.5, ((1, 8),)),
        "decay_bias": scatter_about(seeds[8], (DK, H), 1.0, 4.0, ((0, 8),), jnp.float32),
        "decay_rate": jnp.clip(jnp.exp(math.log(1.5) - 5.0106353 * jax.random.uniform(seeds[9], (DK, H), jnp.float32) ** levels(seeds[9], (DK, H), ((0, 8),), -0.2, 0.2)), 0.01, 1.5),
        "beta_weight": scatter_about(seeds[10], (D, H), D ** -0.5, 0.125, ((0, 4),)),
        "init_state": draw_init_state(jax.random.fold_in(seeds[12], 71), 0),
    }


epsilon = 1e-06

def reference(token_ids, slot_heads, embed_table, query_weight, key_weight, value_weight, decay_down, decay_up, decay_bias, decay_rate, beta_weight, init_state):
    embedded = embed_table[token_ids]
    flat_tokens = embedded.reshape(B * STEPS, D)
    query = jnp.dot(flat_tokens, query_weight.reshape(D, DK * H), preferred_element_type=jnp.float32).reshape(B, STEPS, DK, H)
    query = query * DK ** (-0.5)
    keys = jnp.dot(flat_tokens, key_weight.reshape(D, DK * H), preferred_element_type=jnp.float32).reshape(B, STEPS, DK, H)
    values = jnp.dot(flat_tokens, value_weight.reshape(D, DV * H), preferred_element_type=jnp.float32).reshape(B, STEPS, DV, H)
    low_rank = jnp.dot(flat_tokens, decay_down, preferred_element_type=jnp.float32).astype(jnp.bfloat16)
    gate_input = jnp.dot(low_rank, decay_up.reshape(R, DK * H), preferred_element_type=jnp.float32).reshape(B, STEPS, DK, H)
    alpha = jnp.exp(-decay_rate * jax.nn.softplus(gate_input + decay_bias))
    beta = jax.nn.sigmoid(jnp.dot(flat_tokens, beta_weight, preferred_element_type=jnp.float32)).reshape(B, STEPS, H)
    query = query[..., slot_heads]
    keys = keys[..., slot_heads]
    values = values[..., slot_heads]
    alpha = alpha[..., slot_heads]
    beta = beta[..., slot_heads]
    clip_norm = math.sqrt(DK * DV)
    highest = lax.Precision.HIGHEST
    current = init_state
    outputs = []
    for step in range(STEPS):
        key_now = keys[:, step]
        query_now = query[:, step]
        gate_now = beta[:, step]
        khat = key_now / jnp.sqrt(lax.optimization_barrier(jnp.sum(key_now * key_now, axis=1)) + epsilon)[:, None, :]
        decayed = alpha[:, step][:, :, None, :] * current
        weights_read = jnp.einsum('bih,bijh->bjh', khat, decayed, precision=highest)
        probe = jnp.einsum('bih,bijh->bjh', query_now, decayed, precision=highest)
        cross = lax.optimization_barrier(jnp.sum(khat * query_now, axis=1))
        residue = values[:, step] - weights_read
        updated = decayed + gate_now[:, None, None, :] * khat[:, :, None, :] * residue[:, None, :, :]
        early = probe + (gate_now * cross)[:, None, :] * residue
        norm_total = jnp.sqrt(lax.optimization_barrier(jnp.sum(updated * updated, axis=(1, 2))))
        factor = 1.0 / jnp.maximum(1.0, norm_total / clip_norm)
        current = updated * factor[:, None, None, :]
        outputs.append(early * factor[:, None, :])
    stacked = jnp.stack(outputs, axis=1)
    head_order = jnp.zeros_like(stacked).at[..., slot_heads].set(stacked)
    return (head_order.astype(jnp.bfloat16), current)
```

```python
import math

import jax
import jax.numpy as jnp
from jax import lax
from jax.experimental import pallas as pl
from jax.experimental.pallas import tpu as pltpu
from jax.sharding import PartitionSpec as P

DK = 128
DV = 128
EPSILON = 1e-06
INTERPRET = False

F32 = jnp.float32
BF16 = jnp.bfloat16
BOTH = ("row", "col")
NT = (((1,), (1,)), ((), ()))
NN = (((1,), (0,)), ((), ()))
TN = (((0,), (0,)), ((), ()))


def lanes(shape):
    return lax.broadcasted_iota(jnp.int32, shape, len(shape) - 1)


def rows_of(shape):
    return lax.broadcasted_iota(jnp.int32, shape, len(shape) - 2)


def exchange(array, axis):
    return lax.all_to_all(array, axis, split_axis=0, concat_axis=0, tiled=True)


def pick_kernel(ids_ref, table_ref, out_ref, onehot_ref):
    steps, streams = ids_ref.shape
    feats, vocab = table_ref.shape
    groups = out_ref.shape[0]
    start = lax.axis_index("dp") * vocab
    chunk = onehot_ref.shape[1]
    columns = jnp.broadcast_to((ids_ref[...] - start).astype(F32)[:, None, :], (steps, 8, streams))
    columns = [columns[t].T.astype(jnp.int32)[:, 0:1] for t in range(steps)]
    total = None
    for part in range(vocab // chunk):
        position = lanes((streams, chunk)) + part * chunk
        for t in range(steps):
            hit = columns[t] == position
            onehot_ref[t * streams : (t + 1) * streams, :] = jnp.where(hit, 1.0, 0.0).astype(BF16)
        found = lax.dot_general(
            onehot_ref[...], table_ref[:, part * chunk : (part + 1) * chunk], NT, preferred_element_type=F32
        )
        total = found if total is None else total + found
    wide = jnp.concatenate([total, jnp.zeros((total.shape[0], 128 - feats), F32)], axis=1)
    for t in range(steps):
        block = wide[t * streams : (t + 1) * streams].reshape(groups, 8, 128)
        if t % 2 == 0:
            kept = block
        else:
            pair = jnp.concatenate([kept, block], axis=1)
            out_ref[:, (t - 1) * 8 : (t + 1) * 8, :] = pair.astype(BF16)


def pack_state_kernel(state_ref, out_ref, turned_ref):
    heads = state_ref.shape[3]
    for hi in range(2):
        for i in range(16):
            block = state_ref[hi * 4 : hi * 4 + 4, i].reshape(128, heads)
            turned_ref[pl.ds(hi * 16 + i, heads, stride=32), :] = block.T
    whole = turned_ref[...].reshape(heads, 32, 128)
    upper = whole.astype(BF16)
    out_ref[:, 0:32, :] = upper
    out_ref[:, 32:64, :] = (whole - upper.astype(F32)).astype(BF16)


def add_tokens_kernel(arrived_ref, packed_ref, out_ref, own_ref, sems):
    del packed_ref
    total = arrived_ref[0].astype(F32)
    for k in range(1, arrived_ref.shape[0]):
        total = total + arrived_ref[k].astype(F32)
    own_ref[...] = total.astype(BF16)
    peers = out_ref.shape[0]
    copies = [
        pltpu.make_async_copy(own_ref, out_ref.at[p, 64:96, :], sems.at[p]) for p in range(peers)
    ]
    for copy in copies:
        copy.start()
    for copy in copies:
        copy.wait()


def side_by_side(blocks, width):
    count = (len(blocks) * width + 127) // 128
    tiles = [None] * count
    lane = lanes(blocks[0].shape)
    for k, block in enumerate(blocks):
        at, shift = divmod(k * width, 128)
        rolled = pltpu.roll(block, shift, 1) if shift else block
        low = jnp.where(lane >= shift, rolled, 0.0)
        tiles[at] = low if tiles[at] is None else tiles[at] + low
        if shift + width > 128:
            tiles[at + 1] = jnp.where(lane < shift, rolled, 0.0)
    return jnp.concatenate(tiles, axis=1)


def project_kernel(
    heads_ref, arrived_ref, query_ref, key_ref, value_ref, down_ref, up_ref, bias_ref, rate_ref, beta_ref,
    out_ref, mixed_ref,
):
    col = lax.axis_index("col")
    row = lax.axis_index("row")
    width = query_ref.shape[1] // 8

    def features(first, count):
        blocks = [arrived_ref[first + k, 64:96, :].astype(F32) for k in range(count)]
        return side_by_side(blocks, width)[:, : count * width].astype(BF16)

    own = features(col * 8, 8)
    own_four = jnp.concatenate([own] * 4, axis=0)
    across = features(row * 4, 4)
    across_four = jnp.concatenate([across] * 4, axis=0)

    low = lax.dot_general(own, down_ref[...], NN, preferred_element_type=F32)
    low_upper = low.astype(BF16)
    low_rest = (low - low_upper.astype(F32)).astype(BF16)
    query = lax.dot_general(query_ref[...], own_four, NT, preferred_element_type=F32)
    key = lax.dot_general(key_ref[...], own_four, NT, preferred_element_type=F32)
    gate = lax.dot_general(
        up_ref[...], jnp.concatenate([low_upper] * 4, axis=0), NT, preferred_element_type=F32
    ) + lax.dot_general(
        up_ref[...], jnp.concatenate([low_rest] * 4, axis=0), NT, preferred_element_type=F32
    )
    beta = lax.dot_general(beta_ref[...], own_four, NT, preferred_element_type=F32)
    lane = lanes((32, 128))
    first = jnp.where(col == 0, 1.0, 0.0)
    bias = bias_ref[...].T * first
    rate = rate_ref[...].T * first
    for ch in range(16):
        at = slice(ch * 32, ch * 32 + 32)
        misc = beta
        if ch > 0:
            misc = jnp.broadcast_to(rate[:, ch : ch + 1], (32, 128))
        if ch == 1:
            misc = jnp.where(lane == 97, rate[:, 0:1], misc)
        mixed_ref[at, :] = jnp.where(
            lane < 32,
            query[at],
            jnp.where(lane < 64, key[at], jnp.where(lane < 96, gate[at] + bias[:, ch : ch + 1], misc)),
        )
    value = lax.dot_general(value_ref[...], across_four, NT, preferred_element_type=F32)
    wide = lanes((256, 128))
    mixed_ref[512:768, :] = jnp.where(
        wide < 32,
        value[0:256],
        jnp.where(wide < 64, value[256:512], jnp.where(wide < 96, value[512:768], value[768:1024])),
    )
    for slot in range(32):
        out_ref[slot] = mixed_ref[pl.ds(heads_ref[slot], 24, stride=32), :]


def spread(array, base):
    index = jnp.broadcast_to(lanes((1, 128)) // 32 + base, array.shape)
    return jnp.take_along_axis(array, index, axis=1)


def steps_kernel(arrived_ref, packed_ref, out_ref, state_ref, turned_ref, update_ref, result_ref, scale_ref):
    clip_norm = math.sqrt(DK * DV)
    steps = 4
    lane = lanes((128, 128))
    lane1 = lanes((1, 128))
    mixed = []
    for r in range(8):
        total = arrived_ref[4 * r, 0:16, :]
        for c in range(1, 4):
            total = total + arrived_ref[4 * r + c, 0:16, :]
        mixed.append(total)
    mixed = jnp.concatenate(mixed, axis=0)
    below = pltpu.roll(mixed, 127, 0)
    channel = rows_of((128, 1)) % 16
    rate = jnp.where(channel == 0, below[:, 97:98], mixed[:, 96:97])
    soft = jnp.maximum(mixed, 0.0) + jnp.log1p(jnp.exp(-jnp.abs(mixed)))
    alpha = jnp.exp(-rate * soft)
    key_size = jnp.sum(mixed * mixed, axis=0, keepdims=True)
    inverse = 1.0 / jnp.sqrt(key_size + EPSILON)
    scaled = mixed * jnp.where(lane1 < 32, DK ** (-0.5), inverse)
    cross = jnp.sum(scaled * pltpu.roll(scaled, 96, 1), axis=0, keepdims=True)
    prepared = jnp.where(lane < 64, scaled, alpha)
    write = 1.0 / (1.0 + jnp.exp(-mixed[0:1, :]))

    row8 = rows_of((8, 128))
    lane8 = lanes((8, 128))
    where_tok = (row8 // 2) * 8 + (row8 % 2) * 4 + lane8 // 32
    write8 = jnp.take_along_axis(jnp.broadcast_to(write, (8, 128)), where_tok + 96, axis=1)
    cross8 = jnp.take_along_axis(jnp.broadcast_to(cross, (8, 128)), where_tok, axis=1)

    values = []
    for c in range(4):
        total = arrived_ref[c, 16:24, :]
        for r in range(1, 8):
            total = total + arrived_ref[4 * r + c, 16:24, :]
        values.append(total)
    turned_ref[:, 0:32] = jnp.concatenate(values, axis=0).T
    turned_ref[:, 32:128] = jnp.zeros((128, 96), F32)
    value_rows = [jnp.zeros((8, 128), F32) for _ in range(4)]
    for lo in range(4):
        for octet in range(4):
            part = turned_ref[pl.ds(octet * 32 + lo, 8, stride=4), :]
            target = lo * 32 + octet * 8
            for c in range(4):
                moved = pltpu.roll(part, (target - c * 8) % 128, 1)
                value_rows[c] = jnp.where((lane8 >= target) & (lane8 < target + 8), moved, value_rows[c])

    for hi in range(2):
        for c in range(4):
            for r in range(8):
                upper = packed_ref[4 * r + c, hi * 16 : hi * 16 + 16, :].astype(F32)
                rest = packed_ref[4 * r + c, 32 + hi * 16 : 48 + hi * 16, :].astype(F32)
                state_ref[hi * 4 + c, r * 16 : r * 16 + 16, :] = upper + rest

    for hi in range(2):
        factor = None
        for t in range(steps):
            at = t * 2 + hi
            tok = t * 8 + hi * 4
            alpha_now = spread(prepared, 64 + tok)
            if factor is not None:
                alpha_now = alpha_now * factor
            key_now = spread(prepared, 32 + tok)
            query_now = spread(prepared, tok)
            write_now = write8[at : at + 1]
            cross_now = cross8[at : at + 1] * write_now
            squares = jnp.zeros((1, 128), F32)
            early = []
            for c in range(4):
                decayed = alpha_now * state_ref[hi * 4 + c]
                read = jnp.sum(key_now * decayed, axis=0, keepdims=True)
                probe = jnp.sum(query_now * decayed, axis=0, keepdims=True)
                residue = value_rows[c][at : at + 1] - read
                updated = decayed + key_now * (write_now * residue)
                state_ref[hi * 4 + c] = updated
                squares = squares + jnp.sum(updated * updated, axis=0, keepdims=True)
                update_ref[c, at : at + 1, :] = residue
                early.append(probe + cross_now * residue)
            norm = jnp.zeros((1, 128), F32)
            for lo in range(4):
                inside = lane1 // 32 == lo
                whole = jnp.sum(jnp.where(inside, squares, 0.0), axis=1, keepdims=True)
                norm = jnp.where(inside, whole, norm)
            factor = 1.0 / jnp.maximum(1.0, jnp.sqrt(norm) / clip_norm)
            scale_ref[at : at + 1, :] = factor
            for c in range(4):
                result_ref[c, at : at + 1, :] = early[c] * factor

    combined = jnp.zeros((128, 128), F32)
    for hi in range(2):
        carry = None
        for t in reversed(range(steps)):
            at = t * 2 + hi
            tok = t * 8 + hi * 4
            factor = scale_ref[at : at + 1, :]
            gain = spread(prepared, 32 + tok) * (write8[at : at + 1] * factor)
            decay = spread(prepared, 64 + tok) * factor
            if carry is not None:
                gain = gain * carry
                decay = decay * carry
            carry = decay
            combined = jnp.where(lane % 32 == at, gain, combined)
        combined = jnp.where(lane % 32 == 8 + hi, carry, combined)
    for r in range(8):
        upper = combined[16 * r : 16 * r + 8]
        lower = pltpu.roll(combined[16 * r + 8 : 16 * r + 16], 16, 1)
        both = jnp.where(lane8 % 32 < 16, upper, lower)
        for c in range(4):
            out_ref[4 * r + c, 0:8, :] = update_ref[c]
            out_ref[4 * r + c, 8:16, :] = result_ref[c]
            out_ref[4 * r + c, 16:24, :] = both


def finish_kernel(heads_ref, arrived_ref, state_ref, readout_ref, final_ref, update_ref, gain_ref):
    heads = state_ref.shape[3]
    slot = rows_of((heads, heads))
    head = lanes((heads, heads))
    order = jnp.zeros((heads, heads), F32)
    for s in range(heads):
        order = jnp.where((slot == s) & (head == heads_ref[s]), 1.0, order)
    order = order.astype(BF16)
    for at in range(8):
        t, hi = divmod(at, 2)
        update_ref[at] = arrived_ref[pl.ds(at, heads, stride=24), :].T
        gain_ref[at] = arrived_ref[pl.ds(16 + at, heads, stride=24), :].T
        result = arrived_ref[pl.ds(8 + at, heads, stride=24), :].astype(BF16)
        turned = lax.dot_general(result, order, TN, preferred_element_type=F32).astype(BF16)
        for lo in range(4):
            readout_ref[hi * 4 + lo, t] = turned[lo * 32 : lo * 32 + 32]
    for hi in range(2):
        for lo in range(4):
            updates = [update_ref[t * 2 + hi, lo * 32 : lo * 32 + 32, :] for t in range(4)]
            for i in range(16):
                i_hi, i_lo = divmod(i, 8)
                base = lo * 32 + i_hi * 16
                total = state_ref[hi * 4 + lo, i] * gain_ref[i_lo, base + 8 + hi : base + 9 + hi, :]
                for t in range(4):
                    at = base + t * 2 + hi
                    total = total + gain_ref[i_lo, at : at + 1, :] * updates[t]
                final_ref[hi * 4 + lo, i] = total


VMEM = pl.BlockSpec(memory_space=pltpu.VMEM)
SMEM = pl.BlockSpec(memory_space=pltpu.SMEM)
ANY = pl.BlockSpec(memory_space=pl.ANY)


def shape_of(shape, dtype):
    return jax.ShapeDtypeStruct(shape, dtype)


def shards(
    token_ids, slot_heads, embed_table, query_weight, key_weight, value_weight, decay_down, decay_up, decay_bias,
    decay_rate, beta_weight, init_state,
):
    groups = lax.axis_size("dp")
    ids = token_ids.T
    table = embed_table.T
    picked = pl.pallas_call(
        pick_kernel,
        out_shape=shape_of((groups, 32, 128), BF16),
        in_specs=[VMEM, VMEM],
        out_specs=VMEM,
        scratch_shapes=[pltpu.VMEM((4 * token_ids.shape[0], 1024), BF16)],
        interpret=INTERPRET,
        name="pick",
    )(ids, table)
    arrived = exchange(picked, "dp")
    packed = pl.pallas_call(
        pack_state_kernel,
        out_shape=shape_of((32, 96, 128), BF16),
        in_specs=[VMEM],
        out_specs=VMEM,
        scratch_shapes=[pltpu.VMEM((1024, 128), F32)],
        interpret=INTERPRET,
        name="pack_state",
    )(init_state)
    packed = pl.pallas_call(
        add_tokens_kernel,
        out_shape=shape_of((32, 96, 128), BF16),
        in_specs=[VMEM, ANY],
        out_specs=ANY,
        input_output_aliases={1: 0},
        scratch_shapes=[pltpu.VMEM((32, 128), BF16), pltpu.SemaphoreType.DMA((32,))],
        interpret=INTERPRET,
        name="add_tokens",
    )(arrived, packed)
    packed = exchange(packed, BOTH)
    projected = pl.pallas_call(
        project_kernel,
        out_shape=shape_of((32, 24, 128), F32),
        in_specs=[SMEM] + [VMEM] * 9,
        out_specs=VMEM,
        scratch_shapes=[pltpu.VMEM((768, 128), F32)],
        interpret=INTERPRET,
        name="project",
    )(
        slot_heads,
        packed,
        query_weight.transpose(1, 2, 0).reshape(512, -1),
        key_weight.transpose(1, 2, 0).reshape(512, -1),
        value_weight.transpose(1, 2, 0).reshape(1024, -1),
        decay_down,
        decay_up.transpose(1, 2, 0).reshape(512, -1),
        decay_bias,
        decay_rate,
        beta_weight.T,
    )
    projected = exchange(projected, BOTH)
    stepped = pl.pallas_call(
        steps_kernel,
        out_shape=shape_of((32, 24, 128), F32),
        in_specs=[VMEM, VMEM],
        out_specs=VMEM,
        scratch_shapes=[
            pltpu.VMEM((8, 128, 128), F32),
            pltpu.VMEM((128, 128), F32),
            pltpu.VMEM((4, 8, 128), F32),
            pltpu.VMEM((4, 8, 128), F32),
            pltpu.VMEM((8, 128), F32),
        ],
        interpret=INTERPRET,
        name="steps",
    )(projected, packed)
    stepped = exchange(stepped, BOTH)
    readout, final_state = pl.pallas_call(
        finish_kernel,
        out_shape=(shape_of((8, 4, 32, 32), BF16), shape_of(init_state.shape, F32)),
        in_specs=[SMEM, VMEM, VMEM],
        out_specs=(VMEM, VMEM),
        scratch_shapes=[pltpu.VMEM((8, 128, 32), F32), pltpu.VMEM((8, 128, 32), F32)],
        interpret=INTERPRET,
        name="finish",
    )(slot_heads, stepped.reshape(768, 128), init_state)
    return (readout, final_state)


def solution(mesh):
    in_specs = (
        P(),
        P(),
        P("dp", ("row", "col")),
        P("col", "row", None),
        P("col", "row", None),
        P("row", "col", None),
        P("col", None),
        P(None, "row", None),
        P("row", None),
        P("row", None),
        P("col", None),
        P("dp", "row", "col", None),
    )
    out_specs = (P("dp", None, "col", None), P("dp", "row", "col", None))
    return jax.shard_map(shards, mesh=mesh, in_specs=in_specs, out_specs=out_specs, check_vma=False)
```

```python
import math

import jax
import jax.numpy as jnp
from jax import lax
from jax.experimental import pallas as pl
from jax.experimental.pallas import tpu as pltpu
from jax.sharding import PartitionSpec as P

DK = 128
DV = 128
EPSILON = 1e-06
INTERPRET = False

F32 = jnp.float32
BF16 = jnp.bfloat16
BOTH = ("row", "col")
NT = (((1,), (1,)), ((), ()))
NN = (((1,), (0,)), ((), ()))
TN = (((0,), (0,)), ((), ()))


def lanes(shape):
    return lax.broadcasted_iota(jnp.int32, shape, len(shape) - 1)


def rows_of(shape):
    return lax.broadcasted_iota(jnp.int32, shape, len(shape) - 2)


def exchange(array, axis, shape=None):
    array = lax.all_to_all(array, axis, split_axis=0, concat_axis=0, tiled=True)
    if shape is not None:
        array = array.reshape(shape)
    return kept(array)


def kept(array):
    return array if INTERPRET else pltpu.with_memory_space_constraint(array, pltpu.VMEM)


def pick_kernel(ids_ref, table_ref, out_ref, onehot_ref):
    steps, streams = ids_ref.shape
    feats, vocab = table_ref.shape
    groups = out_ref.shape[0]
    start = lax.axis_index("dp") * vocab
    chunk = onehot_ref.shape[1]
    columns = jnp.broadcast_to((ids_ref[...] - start).astype(F32)[:, None, :], (steps, 8, streams))
    columns = [columns[t].T.astype(jnp.int32)[:, 0:1] for t in range(steps)]
    total = None
    for part in range(vocab // chunk):
        position = lanes((streams, chunk)) + part * chunk
        for t in range(steps):
            hit = columns[t] == position
            onehot_ref[t * streams : (t + 1) * streams, :] = jnp.where(hit, 1.0, 0.0).astype(BF16)
        found = lax.dot_general(
            onehot_ref[...], table_ref[:, part * chunk : (part + 1) * chunk], NT, preferred_element_type=F32
        )
        total = found if total is None else total + found
    wide = jnp.concatenate([total, jnp.zeros((total.shape[0], 128 - feats), F32)], axis=1)
    for t in range(steps):
        block = wide[t * streams : (t + 1) * streams].reshape(groups, 8, 128)
        if t % 2 == 0:
            kept = block
        else:
            pair = jnp.concatenate([kept, block], axis=1)
            out_ref[:, (t - 1) * 8 : (t + 1) * 8, :] = pair.astype(BF16)


def pack_state_kernel(state_ref, early_ref, late_ref, turned_ref):
    heads = state_ref.shape[3]
    for hi in range(2):
        for i in range(16):
            block = state_ref[hi * 4 : hi * 4 + 4, i].reshape(128, heads)
            turned_ref[pl.ds(hi * 16 + i, heads, stride=32), :] = block.T
    whole = turned_ref[...].reshape(heads, 32, 128)
    first = whole[:, 0:16]
    upper = first.astype(BF16)
    early_ref[:, 0:16, :] = upper
    early_ref[:, 16:32, :] = (first - upper.astype(F32)).astype(BF16)
    late_ref[...] = whole[:, 16:32]


def add_tokens_kernel(arrived_ref, early_ref, out_ref):
    total = arrived_ref[0].astype(F32)
    for k in range(1, arrived_ref.shape[0]):
        total = total + arrived_ref[k].astype(F32)
    own = total.astype(BF16)
    out_ref[:, 0:32, :] = early_ref[...]
    for p in range(out_ref.shape[0]):
        out_ref[p, 32:64, :] = own


def side_by_side(blocks, width):
    count = (len(blocks) * width + 127) // 128
    tiles = [None] * count
    lane = lanes(blocks[0].shape)
    for k, block in enumerate(blocks):
        at, shift = divmod(k * width, 128)
        rolled = pltpu.roll(block, shift, 1) if shift else block
        low = jnp.where(lane >= shift, rolled, 0.0)
        tiles[at] = low if tiles[at] is None else tiles[at] + low
        if shift + width > 128:
            tiles[at + 1] = jnp.where(lane < shift, rolled, 0.0)
    return jnp.concatenate(tiles, axis=1)


def project_kernel(
    heads_ref, arrived_ref, query_ref, key_ref, value_ref, down_ref, up_ref, bias_ref, rate_ref, beta_ref,
    late_ref, out_ref, mixed_ref,
):
    col = lax.axis_index("col")
    row = lax.axis_index("row")
    width = query_ref.shape[1] // 8

    def features(first, count):
        blocks = [arrived_ref[first + k, 32:64, :].astype(F32) for k in range(count)]
        return side_by_side(blocks, width)[:, : count * width].astype(BF16)

    own = features(col * 8, 8)
    own_four = jnp.concatenate([own] * 4, axis=0)
    across = features(row * 4, 4)
    across_four = jnp.concatenate([across] * 4, axis=0)

    low = lax.dot_general(own, down_ref[...], NN, preferred_element_type=F32)
    low_upper = low.astype(BF16)
    low_rest = (low - low_upper.astype(F32)).astype(BF16)
    query = lax.dot_general(query_ref[...], own_four, NT, preferred_element_type=F32)
    key = lax.dot_general(key_ref[...], own_four, NT, preferred_element_type=F32)
    gate = lax.dot_general(
        up_ref[...], jnp.concatenate([low_upper] * 4, axis=0), NT, preferred_element_type=F32
    ) + lax.dot_general(
        up_ref[...], jnp.concatenate([low_rest] * 4, axis=0), NT, preferred_element_type=F32
    )
    beta = lax.dot_general(beta_ref[...], own_four, NT, preferred_element_type=F32)
    lane = lanes((32, 128))
    first = jnp.where(col == 0, 1.0, 0.0)
    bias = bias_ref[...].T * first
    rate = rate_ref[...].T * first
    for ch in range(16):
        at = slice(ch * 32, ch * 32 + 32)
        misc = beta
        if ch > 0:
            misc = jnp.broadcast_to(rate[:, ch : ch + 1], (32, 128))
        if ch == 1:
            misc = jnp.where(lane == 97, rate[:, 0:1], misc)
        mixed_ref[at, :] = jnp.where(
            lane < 32,
            query[at],
            jnp.where(lane < 64, key[at], jnp.where(lane < 96, gate[at] + bias[:, ch : ch + 1], misc)),
        )
    value = lax.dot_general(value_ref[...], across_four, NT, preferred_element_type=F32)
    wide = lanes((256, 128))
    mixed_ref[512:768, :] = jnp.where(
        wide < 32,
        value[0:256],
        jnp.where(wide < 64, value[256:512], jnp.where(wide < 96, value[512:768], value[768:1024])),
    )
    for slot in range(32):
        out_ref[slot, 0:24, :] = mixed_ref[pl.ds(heads_ref[slot], 24, stride=32), :]
    out_ref[:, 24:40, :] = late_ref[...]


def spread(array, base):
    index = jnp.broadcast_to(lanes((1, 128)) // 32 + base, array.shape)
    return jnp.take_along_axis(array, index, axis=1)


def steps_kernel(arrived_ref, packed_ref, out_ref, state_ref, turned_ref, update_ref, result_ref, scale_ref):
    clip_norm = math.sqrt(DK * DV)
    steps = 4
    lane = lanes((128, 128))
    lane1 = lanes((1, 128))
    mixed = []
    for r in range(8):
        total = arrived_ref[4 * r, 0:16, :]
        for c in range(1, 4):
            total = total + arrived_ref[4 * r + c, 0:16, :]
        mixed.append(total)
    mixed = jnp.concatenate(mixed, axis=0)
    below = pltpu.roll(mixed, 127, 0)
    channel = rows_of((128, 1)) % 16
    rate = jnp.where(channel == 0, below[:, 97:98], mixed[:, 96:97])
    soft = jnp.maximum(mixed, 0.0) + jnp.log1p(jnp.exp(-jnp.abs(mixed)))
    alpha = jnp.exp(-rate * soft)
    key_size = jnp.sum(mixed * mixed, axis=0, keepdims=True)
    inverse = 1.0 / jnp.sqrt(key_size + EPSILON)
    scaled = mixed * jnp.where(lane1 < 32, DK ** (-0.5), inverse)
    cross = jnp.sum(scaled * pltpu.roll(scaled, 96, 1), axis=0, keepdims=True)
    prepared = jnp.where(lane < 64, scaled, alpha)
    write = 1.0 / (1.0 + jnp.exp(-mixed[0:1, :]))

    row8 = rows_of((8, 128))
    lane8 = lanes((8, 128))
    where_tok = (row8 // 2) * 8 + (row8 % 2) * 4 + lane8 // 32
    write8 = jnp.take_along_axis(jnp.broadcast_to(write, (8, 128)), where_tok + 96, axis=1)
    cross8 = jnp.take_along_axis(jnp.broadcast_to(cross, (8, 128)), where_tok, axis=1)

    values = []
    for c in range(4):
        total = arrived_ref[c, 16:24, :]
        for r in range(1, 8):
            total = total + arrived_ref[4 * r + c, 16:24, :]
        values.append(total)
    turned_ref[:, 0:32] = jnp.concatenate(values, axis=0).T
    turned_ref[:, 32:128] = jnp.zeros((128, 96), F32)
    value_rows = [jnp.zeros((8, 128), F32) for _ in range(4)]
    for lo in range(4):
        for octet in range(4):
            part = turned_ref[pl.ds(octet * 32 + lo, 8, stride=4), :]
            target = lo * 32 + octet * 8
            for c in range(4):
                moved = pltpu.roll(part, (target - c * 8) % 128, 1)
                value_rows[c] = jnp.where((lane8 >= target) & (lane8 < target + 8), moved, value_rows[c])

    for c in range(4):
        for r in range(8):
            at = slice(r * 16, r * 16 + 16)
            upper = packed_ref[4 * r + c, 0:16, :].astype(F32)
            state_ref[c, at, :] = upper + packed_ref[4 * r + c, 16:32, :].astype(F32)
            state_ref[4 + c, at, :] = arrived_ref[4 * r + c, 24:40, :]

    for hi in range(2):
        factor = None
        for t in range(steps):
            at = t * 2 + hi
            tok = t * 8 + hi * 4
            alpha_now = spread(prepared, 64 + tok)
            if factor is not None:
                alpha_now = alpha_now * factor
            key_now = spread(prepared, 32 + tok)
            query_now = spread(prepared, tok)
            write_now = write8[at : at + 1]
            cross_now = cross8[at : at + 1] * write_now
            squares = jnp.zeros((1, 128), F32)
            early = []
            for c in range(4):
                decayed = alpha_now * state_ref[hi * 4 + c]
                read = jnp.sum(key_now * decayed, axis=0, keepdims=True)
                probe = jnp.sum(query_now * decayed, axis=0, keepdims=True)
                residue = value_rows[c][at : at + 1] - read
                updated = decayed + key_now * (write_now * residue)
                state_ref[hi * 4 + c] = updated
                squares = squares + jnp.sum(updated * updated, axis=0, keepdims=True)
                update_ref[c, at : at + 1, :] = residue
                early.append(probe + cross_now * residue)
            norm = jnp.zeros((1, 128), F32)
            for lo in range(4):
                inside = lane1 // 32 == lo
                whole = jnp.sum(jnp.where(inside, squares, 0.0), axis=1, keepdims=True)
                norm = jnp.where(inside, whole, norm)
            factor = 1.0 / jnp.maximum(1.0, jnp.sqrt(norm) / clip_norm)
            scale_ref[at : at + 1, :] = factor
            for c in range(4):
                result_ref[c, at : at + 1, :] = early[c] * factor

    combined = jnp.zeros((128, 128), F32)
    for hi in range(2):
        carry = None
        for t in reversed(range(steps)):
            at = t * 2 + hi
            tok = t * 8 + hi * 4
            factor = scale_ref[at : at + 1, :]
            gain = spread(prepared, 32 + tok) * (write8[at : at + 1] * factor)
            decay = spread(prepared, 64 + tok) * factor
            if carry is not None:
                gain = gain * carry
                decay = decay * carry
            carry = decay
            combined = jnp.where(lane % 32 == at, gain, combined)
        combined = jnp.where(lane % 32 == 8 + hi, carry, combined)
    for r in range(8):
        upper = combined[16 * r : 16 * r + 8]
        lower = pltpu.roll(combined[16 * r + 8 : 16 * r + 16], 16, 1)
        both = jnp.where(lane8 % 32 < 16, upper, lower)
        for c in range(4):
            out_ref[4 * r + c, 0:8, :] = update_ref[c]
            out_ref[4 * r + c, 8:16, :] = result_ref[c]
            out_ref[4 * r + c, 16:24, :] = both


def finish_kernel(heads_ref, arrived_ref, state_ref, readout_ref, final_ref, update_ref, gain_ref):
    heads = state_ref.shape[3]
    slot = rows_of((heads, heads))
    head = lanes((heads, heads))
    order = jnp.zeros((heads, heads), F32)
    for s in range(heads):
        order = jnp.where((slot == s) & (head == heads_ref[s]), 1.0, order)
    order = order.astype(BF16)
    for at in range(8):
        t, hi = divmod(at, 2)
        update_ref[at] = arrived_ref[pl.ds(at, heads, stride=24), :].T
        gain_ref[at] = arrived_ref[pl.ds(16 + at, heads, stride=24), :].T
        result = arrived_ref[pl.ds(8 + at, heads, stride=24), :].astype(BF16)
        turned = lax.dot_general(result, order, TN, preferred_element_type=F32).astype(BF16)
        for lo in range(4):
            readout_ref[hi * 4 + lo, t] = turned[lo * 32 : lo * 32 + 32]
    for hi in range(2):
        for lo in range(4):
            updates = [update_ref[t * 2 + hi, lo * 32 : lo * 32 + 32, :] for t in range(4)]
            for i in range(16):
                i_hi, i_lo = divmod(i, 8)
                base = lo * 32 + i_hi * 16
                total = state_ref[hi * 4 + lo, i] * gain_ref[i_lo, base + 8 + hi : base + 9 + hi, :]
                for t in range(4):
                    at = base + t * 2 + hi
                    total = total + gain_ref[i_lo, at : at + 1, :] * updates[t]
                final_ref[hi * 4 + lo, i] = total


VMEM = pl.BlockSpec(memory_space=pltpu.VMEM)
SMEM = pl.BlockSpec(memory_space=pltpu.SMEM)


def shape_of(shape, dtype):
    return jax.ShapeDtypeStruct(shape, dtype)


def on_chip(shape, dtype):
    return shape_of(shape, dtype) if INTERPRET else pltpu.VMEM(shape, dtype)


def shards(
    token_ids, slot_heads, embed_table, query_weight, key_weight, value_weight, decay_down, decay_up, decay_bias,
    decay_rate, beta_weight, init_state,
):
    groups = lax.axis_size("dp")
    ids = token_ids.T
    table = embed_table.T
    picked = pl.pallas_call(
        pick_kernel,
        out_shape=on_chip((groups, 32, 128), BF16),
        in_specs=[VMEM, VMEM],
        out_specs=VMEM,
        scratch_shapes=[pltpu.VMEM((4 * token_ids.shape[0], 1024), BF16)],
        interpret=INTERPRET,
        name="pick",
    )(ids, table)
    arrived = exchange(picked, "dp")
    early, late = pl.pallas_call(
        pack_state_kernel,
        out_shape=(on_chip((32, 32, 128), BF16), on_chip((32, 16, 128), F32)),
        in_specs=[VMEM],
        out_specs=(VMEM, VMEM),
        scratch_shapes=[pltpu.VMEM((1024, 128), F32)],
        interpret=INTERPRET,
        name="pack_state",
    )(init_state)
    packed = pl.pallas_call(
        add_tokens_kernel,
        out_shape=on_chip((32, 64, 128), BF16),
        in_specs=[VMEM, VMEM],
        out_specs=VMEM,
        interpret=INTERPRET,
        name="add_tokens",
    )(arrived, kept(early))
    packed = exchange(packed, BOTH)
    projected = pl.pallas_call(
        project_kernel,
        out_shape=on_chip((32, 40, 128), F32),
        in_specs=[SMEM] + [VMEM] * 10,
        out_specs=VMEM,
        scratch_shapes=[pltpu.VMEM((768, 128), F32)],
        interpret=INTERPRET,
        name="project",
    )(
        slot_heads,
        packed,
        query_weight.transpose(1, 2, 0).reshape(512, -1),
        key_weight.transpose(1, 2, 0).reshape(512, -1),
        value_weight.transpose(1, 2, 0).reshape(1024, -1),
        decay_down,
        decay_up.transpose(1, 2, 0).reshape(512, -1),
        decay_bias,
        decay_rate,
        beta_weight.T,
        kept(late),
    )
    projected = exchange(projected, BOTH)
    stepped = pl.pallas_call(
        steps_kernel,
        out_shape=on_chip((32, 24, 128), F32),
        in_specs=[VMEM, VMEM],
        out_specs=VMEM,
        scratch_shapes=[
            pltpu.VMEM((8, 128, 128), F32),
            pltpu.VMEM((128, 128), F32),
            pltpu.VMEM((4, 8, 128), F32),
            pltpu.VMEM((4, 8, 128), F32),
            pltpu.VMEM((8, 128), F32),
        ],
        interpret=INTERPRET,
        name="steps",
    )(projected, packed)
    stepped = exchange(stepped, BOTH, (768, 128))
    readout, final_state = pl.pallas_call(
        finish_kernel,
        out_shape=(shape_of((8, 4, 32, 32), BF16), shape_of(init_state.shape, F32)),
        in_specs=[SMEM, VMEM, VMEM],
        out_specs=(VMEM, VMEM),
        scratch_shapes=[pltpu.VMEM((8, 128, 32), F32), pltpu.VMEM((8, 128, 32), F32)],
        interpret=INTERPRET,
        name="finish",
    )(slot_heads, stepped, init_state)
    return (readout, final_state)


def solution(mesh):
    in_specs = (
        P(),
        P(),
        P("dp", ("row", "col")),
        P("col", "row", None),
        P("col", "row", None),
        P("row", "col", None),
        P("col", None),
        P(None, "row", None),
        P("row", None),
        P("row", None),
        P("col", None),
        P("dp", "row", "col", None),
    )
    out_specs = (P("dp", None, "col", None), P("dp", "row", "col", None))
    return jax.shard_map(shards, mesh=mesh, in_specs=in_specs, out_specs=out_specs, check_vma=False)
```

```python
import math

import jax
import jax.numpy as jnp
from jax import lax
from jax.experimental import pallas as pl
from jax.experimental.pallas import tpu as pltpu
from jax.sharding import PartitionSpec as P

DK = 128
DV = 128
EPSILON = 1e-06
INTERPRET = False

F32 = jnp.float32
BF16 = jnp.bfloat16
BOTH = ("row", "col")
NT = (((1,), (1,)), ((), ()))
NN = (((1,), (0,)), ((), ()))
TN = (((0,), (0,)), ((), ()))


def lanes(shape):
    return lax.broadcasted_iota(jnp.int32, shape, len(shape) - 1)


def rows_of(shape):
    return lax.broadcasted_iota(jnp.int32, shape, len(shape) - 2)


def exchange(array, axis, shape=None):
    array = lax.all_to_all(array, axis, split_axis=0, concat_axis=0, tiled=True)
    if shape is not None:
        array = array.reshape(shape)
    return kept(array)


def kept(array):
    return array if INTERPRET else pltpu.with_memory_space_constraint(array, pltpu.VMEM)


def pick_kernel(ids_ref, table_ref, out_ref, onehot_ref):
    steps, streams = ids_ref.shape
    feats, vocab = table_ref.shape
    groups = out_ref.shape[0]
    start = lax.axis_index("dp") * vocab
    local = jnp.broadcast_to((ids_ref[...] - start)[:, None, :], (steps, 8, streams))
    block_of = (local >> 7).astype(F32)
    place_of = (local & 127).astype(F32)
    blocks, places = [], []
    for t in range(steps):
        blocks.append(jnp.broadcast_to(block_of[t].T[:, 0:1], (streams, 128)))
        places.append(place_of[t].T[:, 0:1])
    lane = lanes((streams, 128)).astype(F32)
    blocks = jnp.concatenate(blocks, axis=0).astype(BF16)
    hits = jnp.concatenate([jnp.where(lane == place, 1.0, 0.0) for place in places], axis=0).astype(BF16)
    none = jnp.zeros_like(hits)
    width = onehot_ref.shape[1]
    total = None
    for part in range(vocab // width):
        for k in range(width // 128):
            number = jnp.asarray(part * (width // 128) + k, BF16)
            onehot_ref[:, k * 128 : (k + 1) * 128] = jnp.where(blocks == number, hits, none)
        found = lax.dot_general(
            onehot_ref[...], table_ref[:, part * width : (part + 1) * width], NT, preferred_element_type=F32
        )
        total = found if total is None else total + found
    wide = jnp.concatenate([total, jnp.zeros((total.shape[0], 128 - feats), F32)], axis=1)
    for t in range(steps):
        block = wide[t * streams : (t + 1) * streams].reshape(groups, 8, 128)
        if t % 2 == 0:
            held = block
        else:
            pair = jnp.concatenate([held, block], axis=1)
            out_ref[:, (t - 1) * 8 : (t + 1) * 8, :] = pair.astype(BF16)


def pack_state_kernel(state_ref, early_ref, late_ref, turned_ref):
    heads = state_ref.shape[3]
    for hi in range(2):
        for i in range(16):
            block = state_ref[hi * 4 : hi * 4 + 4, i].reshape(128, heads)
            turned_ref[pl.ds(hi * 16 + i, heads, stride=32), :] = block.T
    whole = turned_ref[...].reshape(heads, 32, 128)
    first = whole[:, 0:16]
    upper = first.astype(BF16)
    early_ref[:, 0:16, :] = upper
    early_ref[:, 16:32, :] = (first - upper.astype(F32)).astype(BF16)
    late_ref[...] = whole[:, 16:32]


def add_tokens_kernel(arrived_ref, early_ref, out_ref):
    total = arrived_ref[0].astype(F32)
    for k in range(1, arrived_ref.shape[0]):
        total = total + arrived_ref[k].astype(F32)
    own = total.astype(BF16)
    out_ref[:, 0:32, :] = early_ref[...]
    for p in range(out_ref.shape[0]):
        out_ref[p, 32:64, :] = own


def side_by_side(blocks, width):
    count = (len(blocks) * width + 127) // 128
    tiles = [None] * count
    lane = lanes(blocks[0].shape)
    for k, block in enumerate(blocks):
        at, shift = divmod(k * width, 128)
        rolled = pltpu.roll(block, shift, 1) if shift else block
        low = jnp.where(lane >= shift, rolled, 0.0)
        tiles[at] = low if tiles[at] is None else tiles[at] + low
        if shift + width > 128:
            tiles[at + 1] = jnp.where(lane < shift, rolled, 0.0)
    return jnp.concatenate(tiles, axis=1)


def project_kernel(
    heads_ref, arrived_ref, query_ref, key_ref, value_ref, down_ref, up_ref, bias_ref, rate_ref, beta_ref,
    late_ref, out_ref, mixed_ref,
):
    col = lax.axis_index("col")
    row = lax.axis_index("row")
    width = query_ref.shape[1] // 8

    def features(first, count):
        blocks = [arrived_ref[first + k, 32:64, :].astype(F32) for k in range(count)]
        return side_by_side(blocks, width)[:, : count * width].astype(BF16)

    own = features(col * 8, 8)
    own_four = jnp.concatenate([own] * 4, axis=0)
    across = features(row * 4, 4)
    across_four = jnp.concatenate([across] * 4, axis=0)

    low = lax.dot_general(own, down_ref[...], NN, preferred_element_type=F32)
    low_upper = low.astype(BF16)
    low_rest = (low - low_upper.astype(F32)).astype(BF16)
    query = lax.dot_general(query_ref[...], own_four, NT, preferred_element_type=F32)
    key = lax.dot_general(key_ref[...], own_four, NT, preferred_element_type=F32)
    gate = lax.dot_general(
        up_ref[...], jnp.concatenate([low_upper] * 4, axis=0), NT, preferred_element_type=F32
    ) + lax.dot_general(
        up_ref[...], jnp.concatenate([low_rest] * 4, axis=0), NT, preferred_element_type=F32
    )
    beta = lax.dot_general(beta_ref[...], own_four, NT, preferred_element_type=F32)
    lane = lanes((32, 128))
    first = jnp.where(col == 0, 1.0, 0.0)
    bias = bias_ref[...].T * first
    rate = rate_ref[...].T * first
    for ch in range(16):
        at = slice(ch * 32, ch * 32 + 32)
        misc = beta
        if ch > 0:
            misc = jnp.broadcast_to(rate[:, ch : ch + 1], (32, 128))
        if ch == 1:
            misc = jnp.where(lane == 97, rate[:, 0:1], misc)
        mixed_ref[at, :] = jnp.where(
            lane < 32,
            query[at],
            jnp.where(lane < 64, key[at], jnp.where(lane < 96, gate[at] + bias[:, ch : ch + 1], misc)),
        )
    value = lax.dot_general(value_ref[...], across_four, NT, preferred_element_type=F32)
    wide = lanes((256, 128))
    mixed_ref[512:768, :] = jnp.where(
        wide < 32,
        value[0:256],
        jnp.where(wide < 64, value[256:512], jnp.where(wide < 96, value[512:768], value[768:1024])),
    )
    for slot in range(32):
        out_ref[slot, 0:24, :] = mixed_ref[pl.ds(heads_ref[slot], 24, stride=32), :]
    out_ref[:, 24:40, :] = late_ref[...]


def spread(array, base):
    index = jnp.broadcast_to(lanes((1, 128)) // 32 + base, array.shape)
    return jnp.take_along_axis(array, index, axis=1)


def steps_kernel(arrived_ref, packed_ref, out_ref, state_ref, turned_ref, update_ref, result_ref, scale_ref):
    clip_norm = math.sqrt(DK * DV)
    steps = 4
    lane = lanes((128, 128))
    lane1 = lanes((1, 128))
    mixed = []
    for r in range(8):
        total = arrived_ref[4 * r, 0:16, :]
        for c in range(1, 4):
            total = total + arrived_ref[4 * r + c, 0:16, :]
        mixed.append(total)
    mixed = jnp.concatenate(mixed, axis=0)
    below = pltpu.roll(mixed, 127, 0)
    channel = rows_of((128, 1)) % 16
    rate = jnp.where(channel == 0, below[:, 97:98], mixed[:, 96:97])
    soft = jnp.maximum(mixed, 0.0) + jnp.log1p(jnp.exp(-jnp.abs(mixed)))
    alpha = jnp.exp(-rate * soft)
    key_size = jnp.sum(mixed * mixed, axis=0, keepdims=True)
    inverse = 1.0 / jnp.sqrt(key_size + EPSILON)
    scaled = mixed * jnp.where(lane1 < 32, DK ** (-0.5), inverse)
    cross = jnp.sum(scaled * pltpu.roll(scaled, 96, 1), axis=0, keepdims=True)
    prepared = jnp.where(lane < 64, scaled, alpha)
    write = 1.0 / (1.0 + jnp.exp(-mixed[0:1, :]))

    row8 = rows_of((8, 128))
    lane8 = lanes((8, 128))
    where_tok = (row8 // 2) * 8 + (row8 % 2) * 4 + lane8 // 32
    write8 = jnp.take_along_axis(jnp.broadcast_to(write, (8, 128)), where_tok + 96, axis=1)
    cross8 = jnp.take_along_axis(jnp.broadcast_to(cross, (8, 128)), where_tok, axis=1)

    values = []
    for c in range(4):
        total = arrived_ref[c, 16:24, :]
        for r in range(1, 8):
            total = total + arrived_ref[4 * r + c, 16:24, :]
        values.append(total)
    turned_ref[:, 0:32] = jnp.concatenate(values, axis=0).T
    turned_ref[:, 32:128] = jnp.zeros((128, 96), F32)
    value_rows = [jnp.zeros((8, 128), F32) for _ in range(4)]
    for lo in range(4):
        for octet in range(4):
            part = turned_ref[pl.ds(octet * 32 + lo, 8, stride=4), :]
            target = lo * 32 + octet * 8
            for c in range(4):
                moved = pltpu.roll(part, (target - c * 8) % 128, 1)
                value_rows[c] = jnp.where((lane8 >= target) & (lane8 < target + 8), moved, value_rows[c])

    for c in range(4):
        for r in range(8):
            at = slice(r * 16, r * 16 + 16)
            upper = packed_ref[4 * r + c, 0:16, :].astype(F32)
            state_ref[c, at, :] = upper + packed_ref[4 * r + c, 16:32, :].astype(F32)
            state_ref[4 + c, at, :] = arrived_ref[4 * r + c, 24:40, :]

    for hi in range(2):
        factor = None
        for t in range(steps):
            at = t * 2 + hi
            tok = t * 8 + hi * 4
            alpha_now = spread(prepared, 64 + tok)
            if factor is not None:
                alpha_now = alpha_now * factor
            key_now = spread(prepared, 32 + tok)
            query_now = spread(prepared, tok)
            write_now = write8[at : at + 1]
            cross_now = cross8[at : at + 1] * write_now
            squares = jnp.zeros((1, 128), F32)
            early = []
            for c in range(4):
                decayed = alpha_now * state_ref[hi * 4 + c]
                read = jnp.sum(key_now * decayed, axis=0, keepdims=True)
                probe = jnp.sum(query_now * decayed, axis=0, keepdims=True)
                residue = value_rows[c][at : at + 1] - read
                updated = decayed + key_now * (write_now * residue)
                state_ref[hi * 4 + c] = updated
                squares = squares + jnp.sum(updated * updated, axis=0, keepdims=True)
                update_ref[c, at : at + 1, :] = residue
                early.append(probe + cross_now * residue)
            norm = jnp.zeros((1, 128), F32)
            for lo in range(4):
                inside = lane1 // 32 == lo
                whole = jnp.sum(jnp.where(inside, squares, 0.0), axis=1, keepdims=True)
                norm = jnp.where(inside, whole, norm)
            factor = 1.0 / jnp.maximum(1.0, jnp.sqrt(norm) / clip_norm)
            scale_ref[at : at + 1, :] = factor
            for c in range(4):
                result_ref[c, at : at + 1, :] = early[c] * factor

    combined = jnp.zeros((128, 128), F32)
    for hi in range(2):
        carry = None
        for t in reversed(range(steps)):
            at = t * 2 + hi
            tok = t * 8 + hi * 4
            factor = scale_ref[at : at + 1, :]
            gain = spread(prepared, 32 + tok) * (write8[at : at + 1] * factor)
            decay = spread(prepared, 64 + tok) * factor
            if carry is not None:
                gain = gain * carry
                decay = decay * carry
            carry = decay
            combined = jnp.where(lane % 32 == at, gain, combined)
        combined = jnp.where(lane % 32 == 8 + hi, carry, combined)
    for r in range(8):
        upper = combined[16 * r : 16 * r + 8]
        lower = pltpu.roll(combined[16 * r + 8 : 16 * r + 16], 16, 1)
        both = jnp.where(lane8 % 32 < 16, upper, lower)
        for c in range(4):
            out_ref[4 * r + c, 0:8, :] = update_ref[c]
            out_ref[4 * r + c, 8:16, :] = result_ref[c]
            out_ref[4 * r + c, 16:24, :] = both


def finish_kernel(heads_ref, arrived_ref, state_ref, readout_ref, final_ref, update_ref, gain_ref, last_ref, sems):
    heads = state_ref.shape[3]
    for at in range(8):
        update_ref[at] = arrived_ref[pl.ds(at, heads, stride=24), :].T
        gain_ref[at] = arrived_ref[pl.ds(16 + at, heads, stride=24), :].T
    copies = []
    for hi in range(2):
        for lo in range(4):
            stream = hi * 4 + lo
            updates = [update_ref[t * 2 + hi, lo * 32 : lo * 32 + 32, :] for t in range(4)]
            for i in range(16):
                i_hi, i_lo = divmod(i, 8)
                base = lo * 32 + i_hi * 16
                total = state_ref[stream, i] * gain_ref[i_lo, base + 8 + hi : base + 9 + hi, :]
                for t in range(4):
                    at = base + t * 2 + hi
                    total = total + gain_ref[i_lo, at : at + 1, :] * updates[t]
                last_ref[stream, i] = total
            copies.append(pltpu.make_async_copy(last_ref.at[stream], final_ref.at[stream], sems.at[stream]))
            copies[-1].start()
    slot = rows_of((heads, heads))
    head = lanes((heads, heads))
    order = jnp.zeros((heads, heads), F32)
    for s in range(heads):
        order = jnp.where((slot == s) & (head == heads_ref[s]), 1.0, order)
    order = order.astype(BF16)
    for at in range(8):
        t, hi = divmod(at, 2)
        result = arrived_ref[pl.ds(8 + at, heads, stride=24), :].astype(BF16)
        turned = lax.dot_general(result, order, TN, preferred_element_type=F32).astype(BF16)
        for lo in range(4):
            readout_ref[hi * 4 + lo, t] = turned[lo * 32 : lo * 32 + 32]
    for copy in copies:
        copy.wait()


VMEM = pl.BlockSpec(memory_space=pltpu.VMEM)
SMEM = pl.BlockSpec(memory_space=pltpu.SMEM)
ANY = pl.BlockSpec(memory_space=pl.ANY)


def shape_of(shape, dtype):
    return jax.ShapeDtypeStruct(shape, dtype)


def on_chip(shape, dtype):
    return shape_of(shape, dtype) if INTERPRET else pltpu.VMEM(shape, dtype)


def shards(
    token_ids, slot_heads, embed_table, query_weight, key_weight, value_weight, decay_down, decay_up, decay_bias,
    decay_rate, beta_weight, init_state,
):
    groups = lax.axis_size("dp")
    state = kept(init_state)
    ids = token_ids.T
    table = embed_table.T
    picked = pl.pallas_call(
        pick_kernel,
        out_shape=on_chip((groups, 32, 128), BF16),
        in_specs=[VMEM, VMEM],
        out_specs=VMEM,
        scratch_shapes=[pltpu.VMEM((4 * token_ids.shape[0], 1024), BF16)],
        interpret=INTERPRET,
        compiler_params=pltpu.CompilerParams(vmem_limit_bytes=16 << 20),
        name="pick",
    )(ids, table)
    arrived = exchange(picked, "dp")
    early, late = pl.pallas_call(
        pack_state_kernel,
        out_shape=(on_chip((32, 32, 128), BF16), on_chip((32, 16, 128), F32)),
        in_specs=[VMEM],
        out_specs=(VMEM, VMEM),
        scratch_shapes=[pltpu.VMEM((1024, 128), F32)],
        interpret=INTERPRET,
        compiler_params=pltpu.CompilerParams(vmem_limit_bytes=16 << 20),
        name="pack_state",
    )(state)
    packed = pl.pallas_call(
        add_tokens_kernel,
        out_shape=on_chip((32, 64, 128), BF16),
        in_specs=[VMEM, VMEM],
        out_specs=VMEM,
        interpret=INTERPRET,
        compiler_params=pltpu.CompilerParams(vmem_limit_bytes=16 << 20),
        name="add_tokens",
    )(arrived, kept(early))
    packed = exchange(packed, BOTH)
    projected = pl.pallas_call(
        project_kernel,
        out_shape=on_chip((32, 40, 128), F32),
        in_specs=[SMEM] + [VMEM] * 10,
        out_specs=VMEM,
        scratch_shapes=[pltpu.VMEM((768, 128), F32)],
        interpret=INTERPRET,
        compiler_params=pltpu.CompilerParams(vmem_limit_bytes=16 << 20),
        name="project",
    )(
        slot_heads,
        packed,
        kept(query_weight.transpose(1, 2, 0).reshape(512, -1)),
        kept(key_weight.transpose(1, 2, 0).reshape(512, -1)),
        kept(value_weight.transpose(1, 2, 0).reshape(1024, -1)),
        kept(decay_down),
        kept(decay_up.transpose(1, 2, 0).reshape(512, -1)),
        decay_bias,
        decay_rate,
        beta_weight.T,
        kept(late),
    )
    projected = exchange(projected, BOTH)
    stepped = pl.pallas_call(
        steps_kernel,
        out_shape=on_chip((32, 24, 128), F32),
        in_specs=[VMEM, VMEM],
        out_specs=VMEM,
        scratch_shapes=[
            pltpu.VMEM((8, 128, 128), F32),
            pltpu.VMEM((128, 128), F32),
            pltpu.VMEM((4, 8, 128), F32),
            pltpu.VMEM((4, 8, 128), F32),
            pltpu.VMEM((8, 128), F32),
        ],
        interpret=INTERPRET,
        compiler_params=pltpu.CompilerParams(vmem_limit_bytes=16 << 20),
        name="steps",
    )(projected, packed)
    stepped = exchange(stepped, BOTH, (768, 128))
    readout, final_state = pl.pallas_call(
        finish_kernel,
        out_shape=(shape_of((8, 4, 32, 32), BF16), shape_of(init_state.shape, F32)),
        in_specs=[SMEM, VMEM, VMEM],
        out_specs=(VMEM, ANY),
        scratch_shapes=[
            pltpu.VMEM((8, 128, 32), F32),
            pltpu.VMEM((8, 128, 32), F32),
            pltpu.VMEM((8, 16, 32, 32), F32),
            pltpu.SemaphoreType.DMA((8,)),
        ],
        interpret=INTERPRET,
        compiler_params=pltpu.CompilerParams(vmem_limit_bytes=16 << 20),
        name="finish",
    )(slot_heads, stepped, state)
    return (readout, final_state)


def solution(mesh):
    in_specs = (
        P(),
        P(),
        P("dp", ("row", "col")),
        P("col", "row", None),
        P("col", "row", None),
        P("row", "col", None),
        P("col", None),
        P(None, "row", None),
        P("row", None),
        P("row", None),
        P("col", None),
        P("dp", "row", "col", None),
    )
    out_specs = (P("dp", None, "col", None), P("dp", "row", "col", None))
    return jax.shard_map(shards, mesh=mesh, in_specs=in_specs, out_specs=out_specs, check_vma=False)
```

```python
import math

import jax
import jax.numpy as jnp
from jax import lax
from jax.experimental import pallas as pl
from jax.experimental.pallas import tpu as pltpu
from jax.sharding import PartitionSpec as P

DK = 128
DV = 128
EPSILON = 1e-06
INTERPRET = False

F32 = jnp.float32
BF16 = jnp.bfloat16
BOTH = ("row", "col")
NT = (((1,), (1,)), ((), ()))
NN = (((1,), (0,)), ((), ()))
TN = (((0,), (0,)), ((), ()))


def lanes(shape):
    return lax.broadcasted_iota(jnp.int32, shape, len(shape) - 1)


def rows_of(shape):
    return lax.broadcasted_iota(jnp.int32, shape, len(shape) - 2)


def exchange(array, axis):
    array = lax.all_to_all(array, axis, split_axis=0, concat_axis=0, tiled=True)
    return kept(array)


def far(array):
    return array if INTERPRET else pltpu.with_memory_space_constraint(array, pltpu.HBM)


def kept(array):
    return array if INTERPRET else pltpu.with_memory_space_constraint(array, pltpu.VMEM)


def pick_kernel(ids_hbm, table_hbm, out_ref, onehot_ref, ids_ref, table_ref, sems):
    steps, streams = ids_ref.shape
    feats, vocab = table_ref.shape
    groups = out_ref.shape[0]
    width = onehot_ref.shape[1]
    ids_copy = pltpu.make_async_copy(ids_hbm, ids_ref, sems.at[0])
    ids_copy.start()
    table_copies = []
    for part in range(vocab // width):
        piece = pl.ds(part * width, width)
        table_copies.append(
            pltpu.make_async_copy(table_hbm.at[:, piece], table_ref.at[:, piece], sems.at[part + 1])
        )
        table_copies[-1].start()
    ids_copy.wait()
    start = lax.axis_index("dp") * vocab
    local = jnp.broadcast_to((ids_ref[...] - start)[:, None, :], (steps, 8, streams))
    block_of = (local >> 7).astype(F32)
    place_of = (local & 127).astype(F32)
    blocks, places = [], []
    for t in range(steps):
        blocks.append(jnp.broadcast_to(block_of[t].T[:, 0:1], (streams, 128)))
        places.append(place_of[t].T[:, 0:1])
    lane = lanes((streams, 128)).astype(F32)
    blocks = jnp.concatenate(blocks, axis=0).astype(BF16)
    hits = jnp.concatenate([jnp.where(lane == place, 1.0, 0.0) for place in places], axis=0).astype(BF16)
    none = jnp.zeros_like(hits)
    total = None
    for part in range(vocab // width):
        for k in range(width // 128):
            number = jnp.asarray(part * (width // 128) + k, BF16)
            onehot_ref[:, k * 128 : (k + 1) * 128] = jnp.where(blocks == number, hits, none)
        table_copies[part].wait()
        found = lax.dot_general(
            onehot_ref[...], table_ref[:, part * width : (part + 1) * width], NT, preferred_element_type=F32
        )
        total = found if total is None else total + found
    wide = jnp.concatenate([total, jnp.zeros((total.shape[0], 128 - feats), F32)], axis=1)
    for t in range(steps):
        block = wide[t * streams : (t + 1) * streams].reshape(groups, 8, 128)
        if t % 2 == 0:
            held = block
        else:
            pair = jnp.concatenate([held, block], axis=1)
            out_ref[:, (t - 1) * 8 : (t + 1) * 8, :] = pair.astype(BF16)


LEVELS = 10
BASE = 2 * LEVELS + 1


def rounded(array):
    return array.astype(BF16).astype(F32)


def left_over(array, upper):
    share = jnp.where(upper == 0.0, 0.0, (array - upper) / jnp.where(upper == 0.0, 1.0, upper))
    return jnp.floor(share * (256.0 * LEVELS) + 0.5)


def joined(pair, both):
    first = jnp.floor(both * (1.0 / BASE) + 0.5)
    second = both - first * BASE
    unit = 1.0 / (256.0 * LEVELS)
    return pair[0:8] * (1.0 + first * unit), pair[8:16] * (1.0 + second * unit)


def pack_state_kernel(state_ref, early_ref, early_rest_ref, late_ref, late_rest_ref, turned_ref):
    heads = state_ref.shape[3]
    for hi in range(2):
        for i in range(16):
            block = state_ref[hi * 4 : hi * 4 + 4, i].reshape(128, heads)
            turned_ref[pl.ds(hi * 16 + i, heads, stride=32), :] = block.T
    whole = turned_ref[...].reshape(heads, 32, 128)
    for hi, (pair_ref, rest_ref) in enumerate(((early_ref, early_rest_ref), (late_ref, late_rest_ref))):
        half = whole[:, hi * 16 : hi * 16 + 16]
        pair_ref[...] = half.astype(BF16)
        left = left_over(half, rounded(half))
        rest_ref[...] = left[:, 0:8] * BASE + left[:, 8:16]


def add_tokens_kernel(arrived_ref, early_ref, early_rest_ref, out_ref):
    own = arrived_ref[0].astype(F32)
    for k in range(1, arrived_ref.shape[0]):
        own = own + arrived_ref[k].astype(F32)
    lane16 = lanes((16, 128))
    lane8 = lanes((8, 128))
    main = jnp.where(lane16 < 64, own[0:16], pltpu.roll(own[16:32], 64, 1)).astype(BF16)
    tail = jnp.zeros((8, 128), F32)
    for k in range(4):
        moved = pltpu.roll(own[8 * k : 8 * k + 8], 64 + 8 * k, 1)
        tail = jnp.where((lane8 >= 8 * k) & (lane8 < 8 * k + 8), moved, tail)
    out_ref[:, 0:16, :] = early_ref[...]
    for p in range(out_ref.shape[0]):
        out_ref[p, 16:32, :] = jnp.concatenate([early_rest_ref[p], tail], axis=0).astype(BF16)
        out_ref[p, 32:48, :] = main


def token_block(arrived_ref, peer):
    main = arrived_ref[peer, 32:48, :].astype(F32)
    tail = arrived_ref[peer, 16:32, :].astype(F32)[8:16]
    lane8 = lanes((8, 128))
    turned = pltpu.roll(main, 64, 1)
    groups = []
    for k in range(4):
        base = main[8 * k : 8 * k + 8] if k < 2 else turned[8 * k - 16 : 8 * k - 8]
        moved = pltpu.roll(tail, 64 - 8 * k, 1)
        groups.append(jnp.where(lane8 < 64, base, jnp.where(lane8 < 72, moved, 0.0)))
    return jnp.concatenate(groups, axis=0)


def side_by_side(blocks, width):
    count = (len(blocks) * width + 127) // 128
    tiles = [None] * count
    lane = lanes(blocks[0].shape)
    for k, block in enumerate(blocks):
        at, shift = divmod(k * width, 128)
        rolled = pltpu.roll(block, shift, 1) if shift else block
        low = jnp.where(lane >= shift, rolled, 0.0)
        tiles[at] = low if tiles[at] is None else tiles[at] + low
        if shift + width > 128:
            tiles[at + 1] = jnp.where(lane < shift, rolled, 0.0)
    return jnp.concatenate(tiles, axis=1)


def project_kernel(
    heads_ref, arrived_ref, query_ref, key_ref, value_ref, down_ref, up_ref, bias_ref, rate_ref, beta_ref,
    late_ref, late_rest_ref, out_ref, mixed_ref,
):
    col = lax.axis_index("col")
    row = lax.axis_index("row")
    width = query_ref.shape[1] // 8

    def features(first, count):
        blocks = [token_block(arrived_ref, first + k) for k in range(count)]
        return side_by_side(blocks, width)[:, : count * width].astype(BF16)

    own = features(col * 8, 8)
    own_four = jnp.concatenate([own] * 4, axis=0)
    across = features(row * 4, 4)
    across_four = jnp.concatenate([across] * 4, axis=0)

    low = lax.dot_general(own, down_ref[...], NN, preferred_element_type=F32)
    low_upper = low.astype(BF16)
    low_rest = (low - low_upper.astype(F32)).astype(BF16)
    query = lax.dot_general(query_ref[...], own_four, NT, preferred_element_type=F32)
    key = lax.dot_general(key_ref[...], own_four, NT, preferred_element_type=F32)
    gate = lax.dot_general(
        up_ref[...], jnp.concatenate([low_upper] * 4, axis=0), NT, preferred_element_type=F32
    ) + lax.dot_general(
        up_ref[...], jnp.concatenate([low_rest] * 4, axis=0), NT, preferred_element_type=F32
    )
    beta = lax.dot_general(beta_ref[...], own_four, NT, preferred_element_type=F32)
    lane = lanes((32, 128))
    first = jnp.where(col == 0, 1.0, 0.0)
    bias = bias_ref[...].T * first
    rate = rate_ref[...].T * first
    for ch in range(16):
        at = slice(ch * 32, ch * 32 + 32)
        misc = beta
        if ch > 0:
            misc = jnp.broadcast_to(rate[:, ch : ch + 1], (32, 128))
        if ch == 1:
            misc = jnp.where(lane == 97, rate[:, 0:1], misc)
        mixed_ref[at, :] = jnp.where(
            lane < 32,
            query[at],
            jnp.where(lane < 64, key[at], jnp.where(lane < 96, gate[at] + bias[:, ch : ch + 1], misc)),
        )
    value = lax.dot_general(value_ref[...], across_four, NT, preferred_element_type=F32)
    wide = lanes((256, 128))
    mixed_ref[512:768, :] = jnp.where(
        wide < 32,
        value[0:256],
        jnp.where(wide < 64, value[256:512], jnp.where(wide < 96, value[512:768], value[768:1024])),
    )
    for slot in range(32):
        sums = mixed_ref[pl.ds(heads_ref[slot], 24, stride=32), :]
        upper = sums[0:16].astype(BF16)
        out_ref[slot, 0:16, :] = upper
        out_ref[slot, 16:32, :] = (sums[0:16] - upper.astype(F32)).astype(BF16)
        out_ref[slot, 48:64, :] = jnp.concatenate([late_rest_ref[slot], sums[16:24]], axis=0).astype(BF16)
    out_ref[:, 32:48, :] = late_ref[...]


def spread(array, base):
    index = jnp.broadcast_to(lanes((1, 128)) // 32 + base, array.shape)
    return jnp.take_along_axis(array, index, axis=1)


def steps_kernel(arrived_ref, packed_ref, out_ref, state_ref, turned_ref, update_ref, result_ref, scale_ref):
    clip_norm = math.sqrt(DK * DV)
    steps = 4
    lane = lanes((128, 128))
    lane1 = lanes((1, 128))
    mixed = []
    for r in range(8):
        total = None
        for c in range(4):
            part = arrived_ref[4 * r + c, 0:16, :].astype(F32) + arrived_ref[4 * r + c, 16:32, :].astype(F32)
            total = part if total is None else total + part
        mixed.append(total)
    mixed = jnp.concatenate(mixed, axis=0)
    below = pltpu.roll(mixed, 127, 0)
    channel = rows_of((128, 1)) % 16
    rate = jnp.where(channel == 0, below[:, 97:98], mixed[:, 96:97])
    soft = jnp.maximum(mixed, 0.0) + jnp.log1p(jnp.exp(-jnp.abs(mixed)))
    alpha = jnp.exp(-rate * soft)
    key_size = jnp.sum(mixed * mixed, axis=0, keepdims=True)
    inverse = 1.0 / jnp.sqrt(key_size + EPSILON)
    scaled = mixed * jnp.where(lane1 < 32, DK ** (-0.5), inverse)
    cross = jnp.sum(scaled * pltpu.roll(scaled, 96, 1), axis=0, keepdims=True)
    prepared = jnp.where(lane < 64, scaled, alpha)
    write = 1.0 / (1.0 + jnp.exp(-mixed[0:1, :]))

    row8 = rows_of((8, 128))
    lane8 = lanes((8, 128))
    where_tok = (row8 // 2) * 8 + (row8 % 2) * 4 + lane8 // 32
    write8 = jnp.take_along_axis(jnp.broadcast_to(write, (8, 128)), where_tok + 96, axis=1)
    cross8 = jnp.take_along_axis(jnp.broadcast_to(cross, (8, 128)), where_tok, axis=1)

    values = []
    for c in range(4):
        total = None
        for r in range(8):
            at = slice(r * 16, r * 16 + 16)
            peer = 4 * r + c
            rest = packed_ref[peer, 16:32, :].astype(F32)[0:8]
            first, second = joined(packed_ref[peer, 0:16, :].astype(F32), rest)
            state_ref[c, at, :] = jnp.concatenate([first, second], axis=0)
            rest = arrived_ref[peer, 48:64, :].astype(F32)
            first, second = joined(arrived_ref[peer, 32:48, :].astype(F32), rest[0:8])
            state_ref[4 + c, at, :] = jnp.concatenate([first, second], axis=0)
            total = rest[8:16] if total is None else total + rest[8:16]
        values.append(total)
    turned_ref[:, 0:32] = jnp.concatenate(values, axis=0).T
    turned_ref[:, 32:128] = jnp.zeros((128, 96), F32)
    value_rows = [jnp.zeros((8, 128), F32) for _ in range(4)]
    for lo in range(4):
        for octet in range(4):
            part = turned_ref[pl.ds(octet * 32 + lo, 8, stride=4), :]
            target = lo * 32 + octet * 8
            for c in range(4):
                moved = pltpu.roll(part, (target - c * 8) % 128, 1)
                value_rows[c] = jnp.where((lane8 >= target) & (lane8 < target + 8), moved, value_rows[c])

    for hi in range(2):
        factor = None
        for t in range(steps):
            at = t * 2 + hi
            tok = t * 8 + hi * 4
            alpha_now = spread(prepared, 64 + tok)
            if factor is not None:
                alpha_now = alpha_now * factor
            key_now = spread(prepared, 32 + tok)
            query_now = spread(prepared, tok)
            write_now = write8[at : at + 1]
            cross_now = cross8[at : at + 1] * write_now
            squares = jnp.zeros((1, 128), F32)
            early = []
            for c in range(4):
                decayed = alpha_now * state_ref[hi * 4 + c]
                read = jnp.sum(key_now * decayed, axis=0, keepdims=True)
                probe = jnp.sum(query_now * decayed, axis=0, keepdims=True)
                residue = value_rows[c][at : at + 1] - read
                updated = decayed + key_now * (write_now * residue)
                state_ref[hi * 4 + c] = updated
                squares = squares + jnp.sum(updated * updated, axis=0, keepdims=True)
                update_ref[c, at : at + 1, :] = residue
                early.append(probe + cross_now * residue)
            norm = jnp.zeros((1, 128), F32)
            for lo in range(4):
                inside = lane1 // 32 == lo
                whole = jnp.sum(jnp.where(inside, squares, 0.0), axis=1, keepdims=True)
                norm = jnp.where(inside, whole, norm)
            factor = 1.0 / jnp.maximum(1.0, jnp.sqrt(norm) / clip_norm)
            scale_ref[at : at + 1, :] = factor
            for c in range(4):
                result_ref[c, at : at + 1, :] = early[c] * factor

    combined = jnp.zeros((128, 128), F32)
    for hi in range(2):
        carry = None
        for t in reversed(range(steps)):
            at = t * 2 + hi
            tok = t * 8 + hi * 4
            factor = scale_ref[at : at + 1, :]
            gain = spread(prepared, 32 + tok) * (write8[at : at + 1] * factor)
            decay = spread(prepared, 64 + tok) * factor
            if carry is not None:
                gain = gain * carry
                decay = decay * carry
            carry = decay
            combined = jnp.where(lane % 32 == at, gain, combined)
        combined = jnp.where(lane % 32 == 8 + hi, carry, combined)
    for r in range(8):
        upper = combined[16 * r : 16 * r + 8]
        lower = pltpu.roll(combined[16 * r + 8 : 16 * r + 16], 16, 1)
        both = jnp.where(lane8 % 32 < 16, upper, lower)
        both_upper = rounded(both)
        for c in range(4):
            update = update_ref[c]
            update_upper = rounded(update)
            peer = 4 * r + c
            out_ref[peer, 0:16, :] = jnp.concatenate([update_upper, update - update_upper], axis=0).astype(BF16)
            out_ref[peer, 16:32, :] = jnp.concatenate([both_upper, both - both_upper], axis=0).astype(BF16)
            out_ref[peer, 32:40, :] = result_ref[c].astype(BF16)


def finish_kernel(
    heads_ref, packed_ref, state_ref, readout_ref, final_ref, arrived_ref, update_ref, gain_ref, last_ref, sems
):
    heads = state_ref.shape[3]
    for s in range(heads):
        update = packed_ref[s, 0:16, :].astype(F32)
        gain = packed_ref[s, 16:32, :].astype(F32)
        arrived_ref[s * 24 : s * 24 + 8, :] = update[0:8] + update[8:16]
        arrived_ref[s * 24 + 8 : s * 24 + 16, :] = packed_ref[s, 32:40, :].astype(F32)
        arrived_ref[s * 24 + 16 : s * 24 + 24, :] = gain[0:8] + gain[8:16]
    for at in range(8):
        update_ref[at] = arrived_ref[pl.ds(at, heads, stride=24), :].T
        gain_ref[at] = arrived_ref[pl.ds(16 + at, heads, stride=24), :].T
    copies = []
    for hi in range(2):
        for lo in range(4):
            stream = hi * 4 + lo
            updates = [update_ref[t * 2 + hi, lo * 32 : lo * 32 + 32, :] for t in range(4)]
            for i in range(16):
                i_hi, i_lo = divmod(i, 8)
                base = lo * 32 + i_hi * 16
                total = state_ref[stream, i] * gain_ref[i_lo, base + 8 + hi : base + 9 + hi, :]
                for t in range(4):
                    at = base + t * 2 + hi
                    total = total + gain_ref[i_lo, at : at + 1, :] * updates[t]
                last_ref[stream, i] = total
            copies.append(pltpu.make_async_copy(last_ref.at[stream], final_ref.at[stream], sems.at[stream]))
            copies[-1].start()
    slot = rows_of((heads, heads))
    head = lanes((heads, heads))
    order = jnp.zeros((heads, heads), F32)
    for s in range(heads):
        order = jnp.where((slot == s) & (head == heads_ref[s]), 1.0, order)
    order = order.astype(BF16)
    for at in range(8):
        t, hi = divmod(at, 2)
        result = arrived_ref[pl.ds(8 + at, heads, stride=24), :].astype(BF16)
        turned = lax.dot_general(result, order, TN, preferred_element_type=F32).astype(BF16)
        for lo in range(4):
            readout_ref[hi * 4 + lo, t] = turned[lo * 32 : lo * 32 + 32]
    for copy in copies:
        copy.wait()


VMEM = pl.BlockSpec(memory_space=pltpu.VMEM)
SMEM = pl.BlockSpec(memory_space=pltpu.SMEM)
ANY = pl.BlockSpec(memory_space=pl.ANY)


def shape_of(shape, dtype):
    return jax.ShapeDtypeStruct(shape, dtype)


def on_chip(shape, dtype):
    return shape_of(shape, dtype) if INTERPRET else pltpu.VMEM(shape, dtype)


def shards(
    token_ids, slot_heads, embed_table, query_weight, key_weight, value_weight, decay_down, decay_up, decay_bias,
    decay_rate, beta_weight, init_state,
):
    groups = lax.axis_size("dp")
    state = kept(init_state)
    ids = token_ids.T
    table = embed_table.T
    picked = pl.pallas_call(
        pick_kernel,
        out_shape=on_chip((groups, 32, 128), BF16),
        in_specs=[ANY, ANY],
        out_specs=VMEM,
        scratch_shapes=[
            pltpu.VMEM((4 * token_ids.shape[0], 1024), BF16),
            pltpu.VMEM(ids.shape, jnp.int32),
            pltpu.VMEM(table.shape, BF16),
            pltpu.SemaphoreType.DMA((1 + table.shape[1] // 1024,)),
        ],
        interpret=INTERPRET,
        compiler_params=pltpu.CompilerParams(vmem_limit_bytes=16 << 20),
        name="pick",
    )(far(ids), far(table))
    arrived = exchange(picked, "dp")
    early, early_rest, late, late_rest = pl.pallas_call(
        pack_state_kernel,
        out_shape=(
            on_chip((32, 16, 128), BF16),
            on_chip((32, 8, 128), F32),
            on_chip((32, 16, 128), BF16),
            on_chip((32, 8, 128), F32),
        ),
        in_specs=[VMEM],
        out_specs=(VMEM, VMEM, VMEM, VMEM),
        scratch_shapes=[pltpu.VMEM((1024, 128), F32)],
        interpret=INTERPRET,
        compiler_params=pltpu.CompilerParams(vmem_limit_bytes=16 << 20),
        name="pack_state",
    )(state)
    packed = pl.pallas_call(
        add_tokens_kernel,
        out_shape=on_chip((32, 48, 128), BF16),
        in_specs=[VMEM, VMEM, VMEM],
        out_specs=VMEM,
        interpret=INTERPRET,
        compiler_params=pltpu.CompilerParams(vmem_limit_bytes=16 << 20),
        name="add_tokens",
    )(arrived, kept(early), kept(early_rest))
    packed = exchange(packed, BOTH)
    projected = pl.pallas_call(
        project_kernel,
        out_shape=on_chip((32, 64, 128), BF16),
        in_specs=[SMEM] + [VMEM] * 11,
        out_specs=VMEM,
        scratch_shapes=[pltpu.VMEM((768, 128), F32)],
        interpret=INTERPRET,
        compiler_params=pltpu.CompilerParams(vmem_limit_bytes=16 << 20),
        name="project",
    )(
        slot_heads,
        packed,
        kept(query_weight.transpose(1, 2, 0).reshape(512, -1)),
        kept(key_weight.transpose(1, 2, 0).reshape(512, -1)),
        kept(value_weight.transpose(1, 2, 0).reshape(1024, -1)),
        kept(decay_down),
        kept(decay_up.transpose(1, 2, 0).reshape(512, -1)),
        decay_bias,
        decay_rate,
        beta_weight.T,
        kept(late),
        kept(late_rest),
    )
    projected = exchange(projected, BOTH)
    stepped = pl.pallas_call(
        steps_kernel,
        out_shape=on_chip((32, 40, 128), BF16),
        in_specs=[VMEM, VMEM],
        out_specs=VMEM,
        scratch_shapes=[
            pltpu.VMEM((8, 128, 128), F32),
            pltpu.VMEM((128, 128), F32),
            pltpu.VMEM((4, 8, 128), F32),
            pltpu.VMEM((4, 8, 128), F32),
            pltpu.VMEM((8, 128), F32),
        ],
        interpret=INTERPRET,
        compiler_params=pltpu.CompilerParams(vmem_limit_bytes=16 << 20),
        name="steps",
    )(projected, packed)
    stepped = exchange(stepped, BOTH)
    readout, final_state = pl.pallas_call(
        finish_kernel,
        out_shape=(shape_of((8, 4, 32, 32), BF16), shape_of(init_state.shape, F32)),
        in_specs=[SMEM, VMEM, VMEM],
        out_specs=(VMEM, ANY),
        scratch_shapes=[
            pltpu.VMEM((768, 128), F32),
            pltpu.VMEM((8, 128, 32), F32),
            pltpu.VMEM((8, 128, 32), F32),
            pltpu.VMEM((8, 16, 32, 32), F32),
            pltpu.SemaphoreType.DMA((8,)),
        ],
        interpret=INTERPRET,
        compiler_params=pltpu.CompilerParams(vmem_limit_bytes=16 << 20),
        name="finish",
    )(slot_heads, stepped, state)
    return (readout, final_state)


def solution(mesh):
    in_specs = (
        P(),
        P(),
        P("dp", ("row", "col")),
        P("col", "row", None),
        P("col", "row", None),
        P("row", "col", None),
        P("col", None),
        P(None, "row", None),
        P("row", None),
        P("row", None),
        P("col", None),
        P("dp", "row", "col", None),
    )
    out_specs = (P("dp", None, "col", None), P("dp", "row", "col", None))
    return jax.shard_map(shards, mesh=mesh, in_specs=in_specs, out_specs=out_specs, check_vma=False)
```

```python
import math

import jax
import jax.numpy as jnp
from jax import lax
from jax.experimental import pallas as pl
from jax.experimental.pallas import tpu as pltpu
from jax.sharding import PartitionSpec as P

DK = 128
DV = 128
EPSILON = 1e-06
INTERPRET = False

F32 = jnp.float32
BF16 = jnp.bfloat16
BOTH = ("row", "col")
NT = (((1,), (1,)), ((), ()))
NN = (((1,), (0,)), ((), ()))
TN = (((0,), (0,)), ((), ()))


def lanes(shape):
    return lax.broadcasted_iota(jnp.int32, shape, len(shape) - 1)


def rows_of(shape):
    return lax.broadcasted_iota(jnp.int32, shape, len(shape) - 2)


def exchange(array, axis):
    array = lax.all_to_all(array, axis, split_axis=0, concat_axis=0, tiled=True)
    return kept(array)


def far(array):
    return array if INTERPRET else pltpu.with_memory_space_constraint(array, pltpu.HBM)


def kept(array):
    return array if INTERPRET else pltpu.with_memory_space_constraint(array, pltpu.VMEM)


def pick_kernel(ids_hbm, table_hbm, out_ref, onehot_ref, ids_ref, table_ref, sems):
    steps, streams = ids_ref.shape
    feats, vocab = table_ref.shape
    groups = out_ref.shape[0]
    ids_copy = pltpu.make_async_copy(ids_hbm, ids_ref, sems.at[0])
    table_copy = pltpu.make_async_copy(table_hbm, table_ref, sems.at[1])
    ids_copy.start()
    table_copy.start()
    ids_copy.wait()
    start = lax.axis_index("dp") * vocab
    wide = jnp.broadcast_to((ids_ref[...] - start).astype(F32)[:, None, :], (steps, 8, streams))
    width = 1024
    for t in range(steps):
        column = wide[t].T.astype(jnp.int32)[:, 0:1]
        for part in range(vocab // width):
            hit = column == lanes((streams, width)) + part * width
            onehot_ref[t * streams : (t + 1) * streams, part * width : (part + 1) * width] = jnp.where(
                hit, 1.0, 0.0
            ).astype(BF16)
    table_copy.wait()
    total = lax.dot_general(onehot_ref[...], table_ref[...], NT, preferred_element_type=F32)
    total = jnp.concatenate([total, jnp.zeros((total.shape[0], 128 - feats), F32)], axis=1)
    for t in range(0, steps, 2):
        pair = [
            total[k * streams : (k + 1) * streams].reshape(groups, 8, 128) for k in (t, t + 1)
        ]
        out_ref[:, t * 8 : t * 8 + 16, :] = jnp.concatenate(pair, axis=1).astype(BF16)


LEVELS = 10
BASE = 2 * LEVELS + 1


def rounded(array):
    return array.astype(BF16).astype(F32)


def left_over(array, upper):
    share = jnp.where(upper == 0.0, 0.0, (array - upper) / jnp.where(upper == 0.0, 1.0, upper))
    return jnp.floor(share * (256.0 * LEVELS) + 0.5)


def joined(pair, both):
    first = jnp.floor(both * (1.0 / BASE) + 0.5)
    second = both - first * BASE
    unit = 1.0 / (256.0 * LEVELS)
    return pair[0:8] * (1.0 + first * unit), pair[8:16] * (1.0 + second * unit)


def left_of_both(array):
    left = left_over(array, rounded(array))
    return left[0:8] * BASE + left[8:16]


def pack_state_kernel(state_ref, early_ref, early_rest_ref, late_ref, late_rest_ref, turned_ref):
    heads = state_ref.shape[3]
    for hi in range(2):
        for i in range(16):
            block = state_ref[hi * 4 : hi * 4 + 4, i].reshape(128, heads)
            turned_ref[pl.ds(hi * 16 + i, heads, stride=32), :] = block.T
    whole = turned_ref[...].reshape(heads, 32, 128)
    for hi, (pair_ref, rest_ref) in enumerate(((early_ref, early_rest_ref), (late_ref, late_rest_ref))):
        half = whole[:, hi * 16 : hi * 16 + 16]
        pair_ref[...] = half.astype(BF16)
        left = left_over(half, rounded(half))
        rest_ref[...] = (left[:, 0:8] * BASE + left[:, 8:16]).astype(rest_ref.dtype)


def add_tokens_kernel(arrived_ref, early_ref, early_rest_ref, out_ref):
    own = arrived_ref[0].astype(F32)
    for k in range(1, arrived_ref.shape[0]):
        own = own + arrived_ref[k].astype(F32)
    lane16 = lanes((16, 128))
    lane8 = lanes((8, 128))
    main = jnp.where(lane16 < 64, own[0:16], pltpu.roll(own[16:32], 64, 1)).astype(BF16)
    tail = jnp.zeros((8, 128), F32)
    for k in range(4):
        moved = pltpu.roll(own[8 * k : 8 * k + 8], 64 + 8 * k, 1)
        tail = jnp.where((lane8 >= 8 * k) & (lane8 < 8 * k + 8), moved, tail)
    out_ref[:, 0:16, :] = early_ref[...]
    for p in range(out_ref.shape[0]):
        out_ref[p, 16:32, :] = jnp.concatenate([early_rest_ref[p], tail], axis=0).astype(BF16)
        out_ref[p, 32:48, :] = main


def token_block(arrived_ref, peer):
    main = arrived_ref[peer, 32:48, :].astype(F32)
    tail = arrived_ref[peer, 16:32, :].astype(F32)[8:16]
    lane8 = lanes((8, 128))
    turned = pltpu.roll(main, 64, 1)
    groups = []
    for k in range(4):
        base = main[8 * k : 8 * k + 8] if k < 2 else turned[8 * k - 16 : 8 * k - 8]
        moved = pltpu.roll(tail, 64 - 8 * k, 1)
        groups.append(jnp.where(lane8 < 64, base, jnp.where(lane8 < 72, moved, 0.0)))
    return jnp.concatenate(groups, axis=0)


def side_by_side(blocks, width):
    count = (len(blocks) * width + 127) // 128
    tiles = [None] * count
    lane = lanes(blocks[0].shape)
    for k, block in enumerate(blocks):
        at, shift = divmod(k * width, 128)
        rolled = pltpu.roll(block, shift, 1) if shift else block
        low = jnp.where(lane >= shift, rolled, 0.0)
        tiles[at] = low if tiles[at] is None else tiles[at] + low
        if shift + width > 128:
            tiles[at + 1] = jnp.where(lane < shift, rolled, 0.0)
    return jnp.concatenate(tiles, axis=1)


def project_kernel(
    heads_ref, arrived_ref, query_ref, key_ref, value_ref, down_ref, up_ref, bias_ref, rate_ref, beta_ref,
    late_ref, late_rest_ref, out_ref, mixed_ref,
):
    col = lax.axis_index("col")
    row = lax.axis_index("row")
    width = query_ref.shape[1] // 8

    def features(first, count):
        blocks = [token_block(arrived_ref, first + k) for k in range(count)]
        return side_by_side(blocks, width)[:, : count * width].astype(BF16)

    own = features(col * 8, 8)
    own_four = jnp.concatenate([own] * 4, axis=0)
    across = features(row * 4, 4)
    across_four = jnp.concatenate([across] * 4, axis=0)

    low = lax.dot_general(own, down_ref[...], NN, preferred_element_type=F32)
    low_upper = low.astype(BF16)
    low_rest = (low - low_upper.astype(F32)).astype(BF16)
    query = lax.dot_general(query_ref[...], own_four, NT, preferred_element_type=F32)
    key = lax.dot_general(key_ref[...], own_four, NT, preferred_element_type=F32)
    gate = lax.dot_general(
        up_ref[...], jnp.concatenate([low_upper] * 4, axis=0), NT, preferred_element_type=F32
    ) + lax.dot_general(
        up_ref[...], jnp.concatenate([low_rest] * 4, axis=0), NT, preferred_element_type=F32
    )
    beta = lax.dot_general(beta_ref[...], own_four, NT, preferred_element_type=F32)
    lane = lanes((32, 128))
    first = jnp.where(col == 0, 1.0, 0.0)
    bias = bias_ref[...].T * first
    rate = rate_ref[...].T * first
    for ch in range(16):
        at = slice(ch * 32, ch * 32 + 32)
        misc = beta
        if ch > 0:
            misc = jnp.broadcast_to(rate[:, ch : ch + 1], (32, 128))
        if ch == 1:
            misc = jnp.where(lane == 97, rate[:, 0:1], misc)
        mixed_ref[at, :] = jnp.where(
            lane < 32,
            query[at],
            jnp.where(lane < 64, key[at], jnp.where(lane < 96, gate[at] + bias[:, ch : ch + 1], misc)),
        )
    value = lax.dot_general(value_ref[...], across_four, NT, preferred_element_type=F32)
    wide = lanes((256, 128))
    mixed_ref[512:768, :] = jnp.where(
        wide < 32,
        value[0:256],
        jnp.where(wide < 64, value[256:512], jnp.where(wide < 96, value[512:768], value[768:1024])),
    )
    for slot in range(32):
        sums = mixed_ref[pl.ds(heads_ref[slot], 24, stride=32), :]
        out_ref[slot, 0:16, :] = sums[0:16].astype(BF16)
        rest = left_of_both(sums[0:16])
        out_ref[slot, 16:32, :] = jnp.concatenate([rest, sums[16:24]], axis=0).astype(BF16)
    out_ref[:, 32:48, :] = late_ref[...]
    out_ref[:, 48:56, :] = late_rest_ref[...]


def spread(array, base):
    index = jnp.broadcast_to(lanes((1, 128)) // 32 + base, array.shape)
    return jnp.take_along_axis(array, index, axis=1)


def steps_kernel(arrived_ref, packed_ref, out_ref, state_ref, turned_ref, update_ref, result_ref, scale_ref):
    clip_norm = math.sqrt(DK * DV)
    steps = 4
    lane = lanes((128, 128))
    lane1 = lanes((1, 128))
    mixed = []
    for r in range(8):
        total = None
        for c in range(4):
            peer = 4 * r + c
            rest = arrived_ref[peer, 16:32, :].astype(F32)[0:8]
            part = jnp.concatenate(joined(arrived_ref[peer, 0:16, :].astype(F32), rest), axis=0)
            total = part if total is None else total + part
        mixed.append(total)
    mixed = jnp.concatenate(mixed, axis=0)
    below = pltpu.roll(mixed, 127, 0)
    channel = rows_of((128, 1)) % 16
    rate = jnp.where(channel == 0, below[:, 97:98], mixed[:, 96:97])
    soft = jnp.maximum(mixed, 0.0) + jnp.log1p(jnp.exp(-jnp.abs(mixed)))
    alpha = jnp.exp(-rate * soft)
    key_size = jnp.sum(mixed * mixed, axis=0, keepdims=True)
    inverse = 1.0 / jnp.sqrt(key_size + EPSILON)
    scaled = mixed * jnp.where(lane1 < 32, DK ** (-0.5), inverse)
    cross = jnp.sum(scaled * pltpu.roll(scaled, 96, 1), axis=0, keepdims=True)
    prepared = jnp.where(lane < 64, scaled, alpha)
    write = 1.0 / (1.0 + jnp.exp(-mixed[0:1, :]))

    row8 = rows_of((8, 128))
    lane8 = lanes((8, 128))
    where_tok = (row8 // 2) * 8 + (row8 % 2) * 4 + lane8 // 32
    write8 = jnp.take_along_axis(jnp.broadcast_to(write, (8, 128)), where_tok + 96, axis=1)
    cross8 = jnp.take_along_axis(jnp.broadcast_to(cross, (8, 128)), where_tok, axis=1)

    values = []
    for c in range(4):
        total = None
        for r in range(8):
            at = slice(r * 16, r * 16 + 16)
            peer = 4 * r + c
            rest = packed_ref[peer, 16:32, :].astype(F32)[0:8]
            first, second = joined(packed_ref[peer, 0:16, :].astype(F32), rest)
            state_ref[c, at, :] = jnp.concatenate([first, second], axis=0)
            rest = arrived_ref[peer, 48:56, :].astype(F32)
            first, second = joined(arrived_ref[peer, 32:48, :].astype(F32), rest)
            state_ref[4 + c, at, :] = jnp.concatenate([first, second], axis=0)
            part = arrived_ref[peer, 16:32, :].astype(F32)[8:16]
            total = part if total is None else total + part
        values.append(total)
    turned_ref[:, 0:32] = jnp.concatenate(values, axis=0).T
    turned_ref[:, 32:128] = jnp.zeros((128, 96), F32)
    value_rows = [jnp.zeros((8, 128), F32) for _ in range(4)]
    for lo in range(4):
        for octet in range(4):
            part = turned_ref[pl.ds(octet * 32 + lo, 8, stride=4), :]
            target = lo * 32 + octet * 8
            for c in range(4):
                moved = pltpu.roll(part, (target - c * 8) % 128, 1)
                value_rows[c] = jnp.where((lane8 >= target) & (lane8 < target + 8), moved, value_rows[c])

    for hi in range(2):
        factor = None
        for t in range(steps):
            at = t * 2 + hi
            tok = t * 8 + hi * 4
            alpha_now = spread(prepared, 64 + tok)
            if factor is not None:
                alpha_now = alpha_now * factor
            key_now = spread(prepared, 32 + tok)
            query_now = spread(prepared, tok)
            write_now = write8[at : at + 1]
            cross_now = cross8[at : at + 1] * write_now
            squares = jnp.zeros((1, 128), F32)
            early = []
            for c in range(4):
                decayed = alpha_now * state_ref[hi * 4 + c]
                read = jnp.sum(key_now * decayed, axis=0, keepdims=True)
                probe = jnp.sum(query_now * decayed, axis=0, keepdims=True)
                residue = value_rows[c][at : at + 1] - read
                updated = decayed + key_now * (write_now * residue)
                state_ref[hi * 4 + c] = updated
                squares = squares + jnp.sum(updated * updated, axis=0, keepdims=True)
                update_ref[c, at : at + 1, :] = residue
                early.append(probe + cross_now * residue)
            norm = jnp.zeros((1, 128), F32)
            for lo in range(4):
                inside = lane1 // 32 == lo
                whole = jnp.sum(jnp.where(inside, squares, 0.0), axis=1, keepdims=True)
                norm = jnp.where(inside, whole, norm)
            factor = 1.0 / jnp.maximum(1.0, jnp.sqrt(norm) / clip_norm)
            scale_ref[at : at + 1, :] = factor
            for c in range(4):
                result_ref[c, at : at + 1, :] = early[c] * factor

    combined = jnp.zeros((128, 128), F32)
    for hi in range(2):
        carry = None
        for t in reversed(range(steps)):
            at = t * 2 + hi
            tok = t * 8 + hi * 4
            factor = scale_ref[at : at + 1, :]
            gain = spread(prepared, 32 + tok) * (write8[at : at + 1] * factor)
            decay = spread(prepared, 64 + tok) * factor
            if carry is not None:
                gain = gain * carry
                decay = decay * carry
            carry = decay
            combined = jnp.where(lane % 32 == at, gain, combined)
        combined = jnp.where(lane % 32 == 8 + hi, carry, combined)
    for r in range(8):
        upper = combined[16 * r : 16 * r + 8]
        lower = pltpu.roll(combined[16 * r + 8 : 16 * r + 16], 16, 1)
        both = jnp.where(lane8 % 32 < 16, upper, lower)
        for c in range(4):
            pair = jnp.concatenate([update_ref[c], both], axis=0)
            rest = jnp.concatenate([left_of_both(pair), result_ref[c]], axis=0)
            out_ref[4 * r + c, 0:16, :] = pair.astype(BF16)
            out_ref[4 * r + c, 16:32, :] = rest.astype(BF16)


def finish_kernel(
    heads_ref, packed_ref, state_ref, readout_hbm, final_hbm,
    arrived_ref, update_ref, gain_ref, readout_ref, final_ref, sems,
):
    heads = state_ref.shape[3]
    for s in range(heads):
        rest = packed_ref[s, 16:32, :].astype(F32)
        update, gain = joined(packed_ref[s, 0:16, :].astype(F32), rest[0:8])
        arrived_ref[s * 24 : s * 24 + 8, :] = update
        arrived_ref[s * 24 + 8 : s * 24 + 16, :] = gain
        arrived_ref[s * 24 + 16 : s * 24 + 24, :] = rest[8:16]
    for at in range(8):
        gain_ref[at] = arrived_ref[pl.ds(8 + at, heads, stride=24), :].T
    copies = []
    for hi in range(2):
        for t in range(4):
            update_ref[t] = arrived_ref[pl.ds(t * 2 + hi, heads, stride=24), :].T
        for lo in range(4):
            stream = hi * 4 + lo
            updates = [update_ref[t, lo * 32 : lo * 32 + 32, :] for t in range(4)]
            for i in range(16):
                i_hi, i_lo = divmod(i, 8)
                base = lo * 32 + i_hi * 16
                total = state_ref[stream, i] * gain_ref[i_lo, base + 8 + hi : base + 9 + hi, :]
                for t in range(4):
                    at = base + t * 2 + hi
                    total = total + gain_ref[i_lo, at : at + 1, :] * updates[t]
                final_ref[stream, i] = total
            copies.append(pltpu.make_async_copy(final_ref.at[stream], final_hbm.at[stream], sems.at[stream]))
            copies[-1].start()
    slot = rows_of((heads, heads))
    head = lanes((heads, heads))
    order = jnp.zeros((heads, heads), F32)
    for s in range(heads):
        order = jnp.where((slot == s) & (head == heads_ref[s]), 1.0, order)
    order = order.astype(BF16)
    for at in range(8):
        t, hi = divmod(at, 2)
        result = arrived_ref[pl.ds(16 + at, heads, stride=24), :].astype(BF16)
        turned = lax.dot_general(result, order, TN, preferred_element_type=F32).astype(BF16)
        for lo in range(4):
            readout_ref[hi * 4 + lo, t] = turned[lo * 32 : lo * 32 + 32]
    copies.append(pltpu.make_async_copy(readout_ref, readout_hbm, sems.at[8]))
    copies[-1].start()
    for copy in copies:
        copy.wait()


VMEM = pl.BlockSpec(memory_space=pltpu.VMEM)
SMEM = pl.BlockSpec(memory_space=pltpu.SMEM)
ANY = pl.BlockSpec(memory_space=pl.ANY)


def shape_of(shape, dtype):
    return jax.ShapeDtypeStruct(shape, dtype)


def on_chip(shape, dtype):
    return shape_of(shape, dtype) if INTERPRET else pltpu.VMEM(shape, dtype)


def shards(
    token_ids, slot_heads, embed_table, query_weight, key_weight, value_weight, decay_down, decay_up, decay_bias,
    decay_rate, beta_weight, init_state,
):
    groups = lax.axis_size("dp")
    state = kept(init_state)
    ids = token_ids.T
    table = embed_table.T
    picked = pl.pallas_call(
        pick_kernel,
        out_shape=on_chip((groups, 32, 128), BF16),
        in_specs=[ANY, ANY],
        out_specs=VMEM,
        scratch_shapes=[
            pltpu.VMEM((4 * token_ids.shape[0], table.shape[1]), BF16),
            pltpu.VMEM(ids.shape, jnp.int32),
            pltpu.VMEM(table.shape, BF16),
            pltpu.SemaphoreType.DMA((2,)),
        ],
        interpret=INTERPRET,
        compiler_params=pltpu.CompilerParams(vmem_limit_bytes=16 << 20),
        name="pick",
    )(far(ids), far(table))
    arrived = exchange(picked, "dp")
    early, early_rest, late, late_rest = pl.pallas_call(
        pack_state_kernel,
        out_shape=(
            on_chip((32, 16, 128), BF16),
            on_chip((32, 8, 128), F32),
            on_chip((32, 16, 128), BF16),
            on_chip((32, 8, 128), BF16),
        ),
        in_specs=[VMEM],
        out_specs=(VMEM, VMEM, VMEM, VMEM),
        scratch_shapes=[pltpu.VMEM((1024, 128), F32)],
        interpret=INTERPRET,
        compiler_params=pltpu.CompilerParams(vmem_limit_bytes=16 << 20),
        name="pack_state",
    )(state)
    packed = pl.pallas_call(
        add_tokens_kernel,
        out_shape=on_chip((32, 48, 128), BF16),
        in_specs=[VMEM, VMEM, VMEM],
        out_specs=VMEM,
        interpret=INTERPRET,
        compiler_params=pltpu.CompilerParams(vmem_limit_bytes=16 << 20),
        name="add_tokens",
    )(arrived, kept(early), kept(early_rest))
    packed = exchange(packed, BOTH)
    projected = pl.pallas_call(
        project_kernel,
        out_shape=on_chip((32, 56, 128), BF16),
        in_specs=[SMEM] + [VMEM] * 11,
        out_specs=VMEM,
        scratch_shapes=[pltpu.VMEM((768, 128), F32)],
        interpret=INTERPRET,
        compiler_params=pltpu.CompilerParams(vmem_limit_bytes=16 << 20),
        name="project",
    )(
        slot_heads,
        packed,
        kept(query_weight.transpose(1, 2, 0).reshape(512, -1)),
        kept(key_weight.transpose(1, 2, 0).reshape(512, -1)),
        kept(value_weight.transpose(1, 2, 0).reshape(1024, -1)),
        kept(decay_down),
        kept(decay_up.transpose(1, 2, 0).reshape(512, -1)),
        decay_bias,
        decay_rate,
        beta_weight.T,
        kept(late),
        kept(late_rest),
    )
    projected = exchange(projected, BOTH)
    stepped = pl.pallas_call(
        steps_kernel,
        out_shape=on_chip((32, 32, 128), BF16),
        in_specs=[VMEM, VMEM],
        out_specs=VMEM,
        scratch_shapes=[
            pltpu.VMEM((8, 128, 128), F32),
            pltpu.VMEM((128, 128), F32),
            pltpu.VMEM((4, 8, 128), F32),
            pltpu.VMEM((4, 8, 128), F32),
            pltpu.VMEM((8, 128), F32),
        ],
        interpret=INTERPRET,
        compiler_params=pltpu.CompilerParams(vmem_limit_bytes=16 << 20),
        name="steps",
    )(projected, packed)
    stepped = exchange(stepped, BOTH)
    readout, final_state = pl.pallas_call(
        finish_kernel,
        out_shape=(shape_of((8, 4, 32, 32), BF16), shape_of(init_state.shape, F32)),
        in_specs=[SMEM, VMEM, VMEM],
        out_specs=(ANY, ANY),
        scratch_shapes=[
            pltpu.VMEM((768, 128), F32),
            pltpu.VMEM((4, 128, 32), F32),
            pltpu.VMEM((8, 128, 32), F32),
            pltpu.VMEM((8, 4, 32, 32), BF16),
            pltpu.VMEM((8, 16, 32, 32), F32),
            pltpu.SemaphoreType.DMA((9,)),
        ],
        interpret=INTERPRET,
        compiler_params=pltpu.CompilerParams(vmem_limit_bytes=16 << 20),
        name="finish",
    )(slot_heads, stepped, state)
    return (readout, final_state)


def solution(mesh):
    in_specs = (
        P(),
        P(),
        P("dp", ("row", "col")),
        P("col", "row", None),
        P("col", "row", None),
        P("row", "col", None),
        P("col", None),
        P(None, "row", None),
        P("row", None),
        P("row", None),
        P("col", None),
        P("dp", "row", "col", None),
    )
    out_specs = (P("dp", None, "col", None), P("dp", "row", "col", None))
    return jax.shard_map(shards, mesh=mesh, in_specs=in_specs, out_specs=out_specs, check_vma=False)
```

```python
import math

import jax
import jax.numpy as jnp
from jax import lax
from jax.experimental import pallas as pl
from jax.experimental.pallas import tpu as pltpu
from jax.sharding import PartitionSpec as P

DK = 128
DV = 128
EPSILON = 1e-06
INTERPRET = False

F32 = jnp.float32
BF16 = jnp.bfloat16
BOTH = ("row", "col")
NT = (((1,), (1,)), ((), ()))
NN = (((1,), (0,)), ((), ()))
TN = (((0,), (0,)), ((), ()))


def lanes(shape):
    return lax.broadcasted_iota(jnp.int32, shape, len(shape) - 1)


def rows_of(shape):
    return lax.broadcasted_iota(jnp.int32, shape, len(shape) - 2)


def exchange(array, axis):
    array = lax.all_to_all(array, axis, split_axis=0, concat_axis=0, tiled=True)
    return kept(array)


def far(array):
    return array if INTERPRET else pltpu.with_memory_space_constraint(array, pltpu.HBM)


def kept(array):
    return array if INTERPRET else pltpu.with_memory_space_constraint(array, pltpu.VMEM)


def pick_kernel(ids_hbm, table_hbm, out_ref, onehot_ref, ids_ref, table_ref, sems):
    steps, streams = ids_ref.shape
    feats, vocab = table_ref.shape
    groups = out_ref.shape[0]
    ids_copy = pltpu.make_async_copy(ids_hbm, ids_ref, sems.at[0])
    table_copy = pltpu.make_async_copy(table_hbm, table_ref, sems.at[1])
    ids_copy.start()
    table_copy.start()
    ids_copy.wait()
    start = lax.axis_index("dp") * vocab
    wide = jnp.broadcast_to((ids_ref[...] - start).astype(F32)[:, None, :], (steps, 8, streams))
    width = 1024
    for t in range(steps):
        column = wide[t].T.astype(jnp.int32)[:, 0:1]
        for part in range(vocab // width):
            hit = column == lanes((streams, width)) + part * width
            onehot_ref[t * streams : (t + 1) * streams, part * width : (part + 1) * width] = jnp.where(
                hit, 1.0, 0.0
            ).astype(BF16)
    table_copy.wait()
    total = lax.dot_general(onehot_ref[...], table_ref[...], NT, preferred_element_type=F32)
    total = jnp.concatenate([total, jnp.zeros((total.shape[0], 128 - feats), F32)], axis=1)
    for t in range(0, steps, 2):
        pair = [
            total[k * streams : (k + 1) * streams].reshape(groups, 8, 128) for k in (t, t + 1)
        ]
        out_ref[:, t * 8 : t * 8 + 16, :] = jnp.concatenate(pair, axis=1).astype(BF16)


LEVELS = 10
BASE = 2 * LEVELS + 1


def rounded(array):
    return array.astype(BF16).astype(F32)


def left_over(array, upper):
    share = jnp.where(upper == 0.0, 0.0, (array - upper) / jnp.where(upper == 0.0, 1.0, upper))
    return jnp.floor(share * (256.0 * LEVELS) + 0.5)


def joined(pair, both):
    first = jnp.floor(both * (1.0 / BASE) + 0.5)
    second = both - first * BASE
    unit = 1.0 / (256.0 * LEVELS)
    return pair[0:8] * (1.0 + first * unit), pair[8:16] * (1.0 + second * unit)


def left_of_both(array):
    left = left_over(array, rounded(array))
    return left[0:8] * BASE + left[8:16]


def pack_state_kernel(state_ref, early_ref, early_rest_ref, late_ref, late_rest_ref, turned_ref):
    heads = state_ref.shape[3]
    for hi in range(2):
        for i in range(16):
            block = state_ref[hi * 4 : hi * 4 + 4, i].reshape(128, heads)
            turned_ref[pl.ds(hi * 16 + i, heads, stride=32), :] = block.T
    whole = turned_ref[...].reshape(heads, 32, 128)
    for hi, (pair_ref, rest_ref) in enumerate(((early_ref, early_rest_ref), (late_ref, late_rest_ref))):
        half = whole[:, hi * 16 : hi * 16 + 16]
        pair_ref[...] = half.astype(BF16)
        left = left_over(half, rounded(half))
        rest_ref[...] = (left[:, 0:8] * BASE + left[:, 8:16]).astype(rest_ref.dtype)


def add_tokens_kernel(arrived_ref, early_ref, early_rest_ref, late_rest_ref, out_ref):
    own = arrived_ref[0].astype(F32)
    for k in range(1, arrived_ref.shape[0]):
        own = own + arrived_ref[k].astype(F32)
    lane16 = lanes((16, 128))
    lane8 = lanes((8, 128))
    main = jnp.where(lane16 < 64, own[0:16], pltpu.roll(own[16:32], 64, 1)).astype(BF16)
    tail = jnp.zeros((8, 128), F32)
    for k in range(4):
        moved = pltpu.roll(own[8 * k : 8 * k + 8], 64 + 8 * k, 1)
        tail = jnp.where((lane8 >= 8 * k) & (lane8 < 8 * k + 8), moved, tail)
    out_ref[:, 0:16, :] = early_ref[...]
    for p in range(out_ref.shape[0]):
        spare = jnp.where(lane8 < 32, tail, late_rest_ref[p])
        out_ref[p, 16:32, :] = jnp.concatenate([early_rest_ref[p], spare], axis=0).astype(BF16)
        out_ref[p, 32:48, :] = main


def token_block(arrived_ref, peer):
    main = arrived_ref[peer, 32:48, :].astype(F32)
    tail = arrived_ref[peer, 16:32, :].astype(F32)[8:16]
    lane8 = lanes((8, 128))
    turned = pltpu.roll(main, 64, 1)
    groups = []
    for k in range(4):
        base = main[8 * k : 8 * k + 8] if k < 2 else turned[8 * k - 16 : 8 * k - 8]
        moved = pltpu.roll(tail, 64 - 8 * k, 1)
        groups.append(jnp.where(lane8 < 64, base, jnp.where(lane8 < 72, moved, 0.0)))
    return jnp.concatenate(groups, axis=0)


def side_by_side(blocks, width):
    count = (len(blocks) * width + 127) // 128
    tiles = [None] * count
    lane = lanes(blocks[0].shape)
    for k, block in enumerate(blocks):
        at, shift = divmod(k * width, 128)
        rolled = pltpu.roll(block, shift, 1) if shift else block
        low = jnp.where(lane >= shift, rolled, 0.0)
        tiles[at] = low if tiles[at] is None else tiles[at] + low
        if shift + width > 128:
            tiles[at + 1] = jnp.where(lane < shift, rolled, 0.0)
    return jnp.concatenate(tiles, axis=1)


def project_kernel(
    heads_ref, arrived_ref, query_ref, key_ref, value_ref, down_ref, up_ref, bias_ref, rate_ref, beta_ref,
    late_ref, late_rest_ref, out_ref, mixed_ref,
):
    col = lax.axis_index("col")
    row = lax.axis_index("row")
    width = query_ref.shape[1] // 8

    def features(first, count):
        blocks = [token_block(arrived_ref, first + k) for k in range(count)]
        return side_by_side(blocks, width)[:, : count * width].astype(BF16)

    own = features(col * 8, 8)
    own_four = jnp.concatenate([own] * 4, axis=0)
    across = features(row * 4, 4)
    across_four = jnp.concatenate([across] * 4, axis=0)

    low = lax.dot_general(own, down_ref[...], NN, preferred_element_type=F32)
    low_upper = low.astype(BF16)
    low_rest = (low - low_upper.astype(F32)).astype(BF16)
    query = lax.dot_general(query_ref[...], own_four, NT, preferred_element_type=F32)
    key = lax.dot_general(key_ref[...], own_four, NT, preferred_element_type=F32)
    gate = lax.dot_general(
        up_ref[...], jnp.concatenate([low_upper] * 4, axis=0), NT, preferred_element_type=F32
    ) + lax.dot_general(
        up_ref[...], jnp.concatenate([low_rest] * 4, axis=0), NT, preferred_element_type=F32
    )
    beta = lax.dot_general(beta_ref[...], own_four, NT, preferred_element_type=F32)
    lane = lanes((32, 128))
    first = jnp.where(col == 0, 1.0, 0.0)
    bias = bias_ref[...].T * first
    rate = rate_ref[...].T * first
    for ch in range(16):
        at = slice(ch * 32, ch * 32 + 32)
        misc = beta
        if 0 < ch < 8:
            misc = jnp.where(lane == 96, rate[:, ch : ch + 1], rate[:, ch + 8 : ch + 9])
        if ch == 1:
            misc = jnp.where(lane == 98, rate[:, 0:1], jnp.where(lane == 99, rate[:, 8:9], misc))
        if ch >= 8:
            misc = jnp.zeros((32, 128), F32)
        mixed_ref[at, :] = jnp.where(
            lane < 32,
            query[at],
            jnp.where(lane < 64, key[at], jnp.where(lane < 96, gate[at] + bias[:, ch : ch + 1], misc)),
        )
    value = lax.dot_general(value_ref[...], across_four, NT, preferred_element_type=F32)
    wide = lanes((256, 128))
    mixed_ref[512:768, :] = jnp.where(
        wide < 32,
        value[0:256],
        jnp.where(wide < 64, value[256:512], jnp.where(wide < 96, value[512:768], value[768:1024])),
    )
    lane8 = lanes((8, 128))
    for slot in range(32):
        sums = mixed_ref[pl.ds(heads_ref[slot], 24, stride=32), :]
        tile = jnp.where(lane8 < 96, sums[8:16], pltpu.roll(late_rest_ref[slot], 96, 1))
        pair = jnp.concatenate([sums[0:8], tile], axis=0)
        out_ref[slot, 0:16, :] = pair.astype(BF16)
        rest = left_of_both(pair)
        out_ref[slot, 16:32, :] = jnp.concatenate([rest, sums[16:24]], axis=0).astype(BF16)
    out_ref[:, 32:48, :] = late_ref[...]


def spread(array, base):
    index = jnp.broadcast_to(lanes((1, 128)) // 32 + base, array.shape)
    return jnp.take_along_axis(array, index, axis=1)


def steps_kernel(arrived_ref, packed_ref, out_ref, state_ref, turned_ref, update_ref, result_ref, scale_ref):
    clip_norm = math.sqrt(DK * DV)
    steps = 4
    lane = lanes((128, 128))
    lane1 = lanes((1, 128))
    mixed = []
    for r in range(8):
        total = None
        for c in range(4):
            peer = 4 * r + c
            rest = arrived_ref[peer, 16:32, :].astype(F32)[0:8]
            part = jnp.concatenate(joined(arrived_ref[peer, 0:16, :].astype(F32), rest), axis=0)
            total = part if total is None else total + part
        mixed.append(total)
    mixed = jnp.concatenate(mixed, axis=0)
    channel = rows_of((128, 1)) % 16
    rate = jnp.where(channel == 0, pltpu.roll(mixed, 127, 0)[:, 98:99], mixed[:, 96:97])
    rate = jnp.where(channel == 8, pltpu.roll(mixed, 7, 0)[:, 99:100], rate)
    rate = jnp.where(channel > 8, pltpu.roll(mixed, 8, 0)[:, 97:98], rate)
    soft = jnp.maximum(mixed, 0.0) + jnp.log1p(jnp.exp(-jnp.abs(mixed)))
    alpha = jnp.exp(-rate * soft)
    key_size = jnp.sum(mixed * mixed, axis=0, keepdims=True)
    inverse = 1.0 / jnp.sqrt(key_size + EPSILON)
    scaled = mixed * jnp.where(lane1 < 32, DK ** (-0.5), inverse)
    cross = jnp.sum(scaled * pltpu.roll(scaled, 96, 1), axis=0, keepdims=True)
    prepared = jnp.where(lane < 64, scaled, alpha)
    write = 1.0 / (1.0 + jnp.exp(-mixed[0:1, :]))

    row8 = rows_of((8, 128))
    lane8 = lanes((8, 128))
    where_tok = (row8 // 2) * 8 + (row8 % 2) * 4 + lane8 // 32
    write8 = jnp.take_along_axis(jnp.broadcast_to(write, (8, 128)), where_tok + 96, axis=1)
    cross8 = jnp.take_along_axis(jnp.broadcast_to(cross, (8, 128)), where_tok, axis=1)

    values = []
    for c in range(4):
        total = None
        for r in range(8):
            at = slice(r * 16, r * 16 + 16)
            peer = 4 * r + c
            rest = packed_ref[peer, 16:32, :].astype(F32)
            first, second = joined(packed_ref[peer, 0:16, :].astype(F32), rest[0:8])
            state_ref[c, at, :] = jnp.concatenate([first, second], axis=0)
            tile = arrived_ref[peer, 0:16, :].astype(F32)[8:16]
            rest = jnp.where(lane8 < 32, pltpu.roll(tile, 32, 1), rest[8:16])
            first, second = joined(arrived_ref[peer, 32:48, :].astype(F32), rest)
            state_ref[4 + c, at, :] = jnp.concatenate([first, second], axis=0)
            part = arrived_ref[peer, 16:32, :].astype(F32)[8:16]
            total = part if total is None else total + part
        values.append(total)
    turned_ref[:, 0:32] = jnp.concatenate(values, axis=0).T
    turned_ref[:, 32:128] = jnp.zeros((128, 96), F32)
    value_rows = [jnp.zeros((8, 128), F32) for _ in range(4)]
    for lo in range(4):
        for octet in range(4):
            part = turned_ref[pl.ds(octet * 32 + lo, 8, stride=4), :]
            target = lo * 32 + octet * 8
            for c in range(4):
                moved = pltpu.roll(part, (target - c * 8) % 128, 1)
                value_rows[c] = jnp.where((lane8 >= target) & (lane8 < target + 8), moved, value_rows[c])

    for hi in range(2):
        factor = None
        for t in range(steps):
            at = t * 2 + hi
            tok = t * 8 + hi * 4
            alpha_now = spread(prepared, 64 + tok)
            if factor is not None:
                alpha_now = alpha_now * factor
            key_now = spread(prepared, 32 + tok)
            query_now = spread(prepared, tok)
            write_now = write8[at : at + 1]
            cross_now = cross8[at : at + 1] * write_now
            squares = jnp.zeros((1, 128), F32)
            early = []
            for c in range(4):
                decayed = alpha_now * state_ref[hi * 4 + c]
                read = jnp.sum(key_now * decayed, axis=0, keepdims=True)
                probe = jnp.sum(query_now * decayed, axis=0, keepdims=True)
                residue = value_rows[c][at : at + 1] - read
                updated = decayed + key_now * (write_now * residue)
                state_ref[hi * 4 + c] = updated
                squares = squares + jnp.sum(updated * updated, axis=0, keepdims=True)
                update_ref[c, at : at + 1, :] = residue
                early.append(probe + cross_now * residue)
            norm = jnp.zeros((1, 128), F32)
            for lo in range(4):
                inside = lane1 // 32 == lo
                whole = jnp.sum(jnp.where(inside, squares, 0.0), axis=1, keepdims=True)
                norm = jnp.where(inside, whole, norm)
            factor = 1.0 / jnp.maximum(1.0, jnp.sqrt(norm) / clip_norm)
            scale_ref[at : at + 1, :] = factor
            for c in range(4):
                result_ref[c, at : at + 1, :] = early[c] * factor

    combined = jnp.zeros((128, 128), F32)
    for hi in range(2):
        carry = None
        for t in reversed(range(steps)):
            at = t * 2 + hi
            tok = t * 8 + hi * 4
            factor = scale_ref[at : at + 1, :]
            gain = spread(prepared, 32 + tok) * (write8[at : at + 1] * factor)
            decay = spread(prepared, 64 + tok) * factor
            if carry is not None:
                gain = gain * carry
                decay = decay * carry
            carry = decay
            combined = jnp.where(lane % 32 == at, gain, combined)
        combined = jnp.where(lane % 32 == 8 + hi, carry, combined)
    for r in range(8):
        upper = combined[16 * r : 16 * r + 8]
        lower = pltpu.roll(combined[16 * r + 8 : 16 * r + 16], 16, 1)
        both = jnp.where(lane8 % 32 < 16, upper, lower)
        for c in range(4):
            pair = jnp.concatenate([update_ref[c], both], axis=0)
            rest = jnp.concatenate([left_of_both(pair), result_ref[c]], axis=0)
            out_ref[4 * r + c, 0:16, :] = pair.astype(BF16)
            out_ref[4 * r + c, 16:32, :] = rest.astype(BF16)


def finish_kernel(
    heads_ref, packed_ref, state_ref, readout_hbm, final_hbm,
    arrived_ref, update_ref, gain_ref, readout_ref, final_ref, sems,
):
    heads = state_ref.shape[3]
    for s in range(heads):
        rest = packed_ref[s, 16:32, :].astype(F32)
        update, gain = joined(packed_ref[s, 0:16, :].astype(F32), rest[0:8])
        arrived_ref[s * 24 : s * 24 + 8, :] = update
        arrived_ref[s * 24 + 8 : s * 24 + 16, :] = gain
        arrived_ref[s * 24 + 16 : s * 24 + 24, :] = rest[8:16]
    for at in range(8):
        gain_ref[at] = arrived_ref[pl.ds(8 + at, heads, stride=24), :].T
    copies = []
    for hi in range(2):
        for t in range(4):
            update_ref[t] = arrived_ref[pl.ds(t * 2 + hi, heads, stride=24), :].T
        for lo in range(4):
            stream = hi * 4 + lo
            updates = [update_ref[t, lo * 32 : lo * 32 + 32, :] for t in range(4)]
            for i in range(16):
                i_hi, i_lo = divmod(i, 8)
                base = lo * 32 + i_hi * 16
                total = state_ref[stream, i] * gain_ref[i_lo, base + 8 + hi : base + 9 + hi, :]
                for t in range(4):
                    at = base + t * 2 + hi
                    total = total + gain_ref[i_lo, at : at + 1, :] * updates[t]
                final_ref[stream, i] = total
            copies.append(pltpu.make_async_copy(final_ref.at[stream], final_hbm.at[stream], sems.at[stream]))
            copies[-1].start()
    slot = rows_of((heads, heads))
    head = lanes((heads, heads))
    order = jnp.zeros((heads, heads), F32)
    for s in range(heads):
        order = jnp.where((slot == s) & (head == heads_ref[s]), 1.0, order)
    order = order.astype(BF16)
    for at in range(8):
        t, hi = divmod(at, 2)
        result = arrived_ref[pl.ds(16 + at, heads, stride=24), :].astype(BF16)
        turned = lax.dot_general(result, order, TN, preferred_element_type=F32).astype(BF16)
        for lo in range(4):
            readout_ref[hi * 4 + lo, t] = turned[lo * 32 : lo * 32 + 32]
    copies.append(pltpu.make_async_copy(readout_ref, readout_hbm, sems.at[8]))
    copies[-1].start()
    for copy in copies:
        copy.wait()


VMEM = pl.BlockSpec(memory_space=pltpu.VMEM)
SMEM = pl.BlockSpec(memory_space=pltpu.SMEM)
ANY = pl.BlockSpec(memory_space=pl.ANY)


def shape_of(shape, dtype):
    return jax.ShapeDtypeStruct(shape, dtype)


def on_chip(shape, dtype):
    return shape_of(shape, dtype) if INTERPRET else pltpu.VMEM(shape, dtype)


def shards(
    token_ids, slot_heads, embed_table, query_weight, key_weight, value_weight, decay_down, decay_up, decay_bias,
    decay_rate, beta_weight, init_state,
):
    groups = lax.axis_size("dp")
    state = kept(init_state)
    ids = token_ids.T
    table = embed_table.T
    picked = pl.pallas_call(
        pick_kernel,
        out_shape=on_chip((groups, 32, 128), BF16),
        in_specs=[ANY, ANY],
        out_specs=VMEM,
        scratch_shapes=[
            pltpu.VMEM((4 * token_ids.shape[0], table.shape[1]), BF16),
            pltpu.VMEM(ids.shape, jnp.int32),
            pltpu.VMEM(table.shape, BF16),
            pltpu.SemaphoreType.DMA((2,)),
        ],
        interpret=INTERPRET,
        compiler_params=pltpu.CompilerParams(vmem_limit_bytes=16 << 20),
        name="pick",
    )(far(ids), far(table))
    arrived = exchange(picked, "dp")
    early, early_rest, late, late_rest = pl.pallas_call(
        pack_state_kernel,
        out_shape=(
            on_chip((32, 16, 128), BF16),
            on_chip((32, 8, 128), F32),
            on_chip((32, 16, 128), BF16),
            on_chip((32, 8, 128), F32),
        ),
        in_specs=[VMEM],
        out_specs=(VMEM, VMEM, VMEM, VMEM),
        scratch_shapes=[pltpu.VMEM((1024, 128), F32)],
        interpret=INTERPRET,
        compiler_params=pltpu.CompilerParams(vmem_limit_bytes=16 << 20),
        name="pack_state",
    )(state)
    packed = pl.pallas_call(
        add_tokens_kernel,
        out_shape=on_chip((32, 48, 128), BF16),
        in_specs=[VMEM, VMEM, VMEM, VMEM],
        out_specs=VMEM,
        interpret=INTERPRET,
        compiler_params=pltpu.CompilerParams(vmem_limit_bytes=16 << 20),
        name="add_tokens",
    )(arrived, kept(early), kept(early_rest), kept(late_rest))
    packed = exchange(packed, BOTH)
    projected = pl.pallas_call(
        project_kernel,
        out_shape=on_chip((32, 48, 128), BF16),
        in_specs=[SMEM] + [VMEM] * 11,
        out_specs=VMEM,
        scratch_shapes=[pltpu.VMEM((768, 128), F32)],
        interpret=INTERPRET,
        compiler_params=pltpu.CompilerParams(vmem_limit_bytes=16 << 20),
        name="project",
    )(
        slot_heads,
        packed,
        kept(query_weight.transpose(1, 2, 0).reshape(512, -1)),
        kept(key_weight.transpose(1, 2, 0).reshape(512, -1)),
        kept(value_weight.transpose(1, 2, 0).reshape(1024, -1)),
        kept(decay_down),
        kept(decay_up.transpose(1, 2, 0).reshape(512, -1)),
        decay_bias,
        decay_rate,
        beta_weight.T,
        kept(late),
        kept(late_rest),
    )
    projected = exchange(projected, BOTH)
    stepped = pl.pallas_call(
        steps_kernel,
        out_shape=on_chip((32, 32, 128), BF16),
        in_specs=[VMEM, VMEM],
        out_specs=VMEM,
        scratch_shapes=[
            pltpu.VMEM((8, 128, 128), F32),
            pltpu.VMEM((128, 128), F32),
            pltpu.VMEM((4, 8, 128), F32),
            pltpu.VMEM((4, 8, 128), F32),
            pltpu.VMEM((8, 128), F32),
        ],
        interpret=INTERPRET,
        compiler_params=pltpu.CompilerParams(vmem_limit_bytes=16 << 20),
        name="steps",
    )(projected, packed)
    stepped = exchange(stepped, BOTH)
    readout, final_state = pl.pallas_call(
        finish_kernel,
        out_shape=(shape_of((8, 4, 32, 32), BF16), shape_of(init_state.shape, F32)),
        in_specs=[SMEM, VMEM, VMEM],
        out_specs=(ANY, ANY),
        scratch_shapes=[
            pltpu.VMEM((768, 128), F32),
            pltpu.VMEM((4, 128, 32), F32),
            pltpu.VMEM((8, 128, 32), F32),
            pltpu.VMEM((8, 4, 32, 32), BF16),
            pltpu.VMEM((8, 16, 32, 32), F32),
            pltpu.SemaphoreType.DMA((9,)),
        ],
        interpret=INTERPRET,
        compiler_params=pltpu.CompilerParams(vmem_limit_bytes=16 << 20),
        name="finish",
    )(slot_heads, stepped, state)
    return (readout, final_state)


def solution(mesh):
    in_specs = (
        P(),
        P(),
        P("dp", ("row", "col")),
        P("col", "row", None),
        P("col", "row", None),
        P("row", "col", None),
        P("col", None),
        P(None, "row", None),
        P("row", None),
        P("row", None),
        P("col", None),
        P("dp", "row", "col", None),
    )
    out_specs = (P("dp", None, "col", None), P("dp", "row", "col", None))
    return jax.shard_map(shards, mesh=mesh, in_specs=in_specs, out_specs=out_specs, check_vma=False)
```

```python
import math

import jax
import jax.numpy as jnp
from jax import lax
from jax.experimental import pallas as pl
from jax.experimental.pallas import tpu as pltpu
from jax.sharding import PartitionSpec as P

DK = 128
DV = 128
EPSILON = 1e-06
INTERPRET = False

F32 = jnp.float32
BF16 = jnp.bfloat16
BOTH = ("row", "col")
NT = (((1,), (1,)), ((), ()))
NN = (((1,), (0,)), ((), ()))
TN = (((0,), (0,)), ((), ()))


def lanes(shape):
    return lax.broadcasted_iota(jnp.int32, shape, len(shape) - 1)


def rows_of(shape):
    return lax.broadcasted_iota(jnp.int32, shape, len(shape) - 2)


def exchange(array, axis):
    array = lax.all_to_all(array, axis, split_axis=0, concat_axis=0, tiled=True)
    return kept(array)


def far(array):
    return array if INTERPRET else pltpu.with_memory_space_constraint(array, pltpu.HBM)


def kept(array):
    return array if INTERPRET else pltpu.with_memory_space_constraint(array, pltpu.VMEM)


def pick_kernel(ids_hbm, table_hbm, out_ref, onehot_ref, ids_ref, table_ref, sems):
    steps, streams = ids_ref.shape
    feats, vocab = table_ref.shape
    groups = out_ref.shape[0]
    ids_copy = pltpu.make_async_copy(ids_hbm, ids_ref, sems.at[0])
    table_copy = pltpu.make_async_copy(table_hbm, table_ref, sems.at[1])
    ids_copy.start()
    table_copy.start()
    ids_copy.wait()
    table_copy.wait()
    start = lax.axis_index("dp") * vocab
    wide = jnp.broadcast_to((ids_ref[...] - start).astype(F32)[:, None, :], (steps, 8, streams))
    columns = [wide[t].T.astype(jnp.int32)[:, 0:1] for t in range(steps)]
    width = 1024
    total = None
    for part in range(vocab // width):
        across = slice(part * width, (part + 1) * width)
        for t in range(steps):
            hit = columns[t] == lanes((streams, width)) + part * width
            onehot_ref[t * streams : (t + 1) * streams, across] = jnp.where(hit, 1.0, 0.0).astype(BF16)
        found = lax.dot_general(onehot_ref[:, across], table_ref[:, across], NT, preferred_element_type=F32)
        total = found if total is None else total + found
    total = jnp.concatenate([total, jnp.zeros((total.shape[0], 128 - feats), F32)], axis=1)
    steps_rows = [total[t * streams : (t + 1) * streams] for t in range(steps)]
    lane = lanes((streams, 128))
    tail = jnp.zeros((streams, 128), F32)
    for t in range(steps):
        moved = pltpu.roll(steps_rows[t], 64 + 8 * t, 1)
        tail = jnp.where((lane >= 8 * t) & (lane < 8 * t + 8), moved, tail)
    main = [jnp.where(lane < 64, steps_rows[t], pltpu.roll(steps_rows[t + 2], 64, 1)) for t in range(2)]
    main = [part.reshape(groups, 8, 128) for part in main]
    out_ref[:, 0:16, :] = jnp.concatenate(main, axis=1).astype(BF16)
    out_ref[:, 16:24, :] = tail.reshape(groups, 8, 128).astype(BF16)


LEVELS = 10
BASE = 2 * LEVELS + 1


def rounded(array):
    return array.astype(BF16).astype(F32)


def left_over(array, upper):
    share = jnp.where(upper == 0.0, 0.0, (array - upper) / jnp.where(upper == 0.0, 1.0, upper))
    return jnp.floor(share * (256.0 * LEVELS) + 0.5)


def joined(pair, both):
    first = jnp.floor(both * (1.0 / BASE) + 0.5)
    second = both - first * BASE
    unit = 1.0 / (256.0 * LEVELS)
    return pair[0:8] * (1.0 + first * unit), pair[8:16] * (1.0 + second * unit)


def left_of_both(array):
    left = left_over(array, rounded(array))
    return left[0:8] * BASE + left[8:16]


def pack_state_kernel(state_ref, early_ref, early_rest_ref, late_ref, late_rest_ref, turned_ref):
    heads = state_ref.shape[3]
    for hi in range(2):
        for i in range(16):
            block = state_ref[hi * 4 : hi * 4 + 4, i].reshape(128, heads)
            turned_ref[pl.ds(hi * 16 + i, heads, stride=32), :] = block.T
    whole = turned_ref[...].reshape(heads, 32, 128)
    for hi, (pair_ref, rest_ref) in enumerate(((early_ref, early_rest_ref), (late_ref, late_rest_ref))):
        half = whole[:, hi * 16 : hi * 16 + 16]
        pair_ref[...] = half.astype(BF16)
        left = left_over(half, rounded(half))
        rest_ref[...] = (left[:, 0:8] * BASE + left[:, 8:16]).astype(rest_ref.dtype)


def add_tokens_kernel(arrived_ref, early_ref, early_rest_ref, late_rest_ref, out_ref):
    own = arrived_ref[0].astype(F32)
    for k in range(1, arrived_ref.shape[0]):
        own = own + arrived_ref[k].astype(F32)
    lane8 = lanes((8, 128))
    main = own[0:16].astype(BF16)
    tail = own[16:24]
    out_ref[:, 0:16, :] = early_ref[...]
    for p in range(out_ref.shape[0]):
        spare = jnp.where(lane8 < 32, tail, late_rest_ref[p])
        out_ref[p, 16:32, :] = jnp.concatenate([early_rest_ref[p], spare], axis=0).astype(BF16)
        out_ref[p, 32:48, :] = main


def token_block(arrived_ref, peer):
    main = arrived_ref[peer, 32:48, :].astype(F32)
    tail = arrived_ref[peer, 16:32, :].astype(F32)[8:16]
    lane8 = lanes((8, 128))
    turned = pltpu.roll(main, 64, 1)
    groups = []
    for k in range(4):
        base = main[8 * k : 8 * k + 8] if k < 2 else turned[8 * k - 16 : 8 * k - 8]
        moved = pltpu.roll(tail, 64 - 8 * k, 1)
        groups.append(jnp.where(lane8 < 64, base, jnp.where(lane8 < 72, moved, 0.0)))
    return jnp.concatenate(groups, axis=0)


def side_by_side(blocks, width):
    count = (len(blocks) * width + 127) // 128
    tiles = [None] * count
    lane = lanes(blocks[0].shape)
    for k, block in enumerate(blocks):
        at, shift = divmod(k * width, 128)
        rolled = pltpu.roll(block, shift, 1) if shift else block
        low = jnp.where(lane >= shift, rolled, 0.0)
        tiles[at] = low if tiles[at] is None else tiles[at] + low
        if shift + width > 128:
            tiles[at + 1] = jnp.where(lane < shift, rolled, 0.0)
    return jnp.concatenate(tiles, axis=1)


def project_kernel(
    heads_ref, arrived_ref, query_ref, key_ref, value_ref, down_ref, up_ref, bias_ref, rate_ref, beta_ref,
    late_ref, late_rest_ref, out_ref, mixed_ref,
):
    col = lax.axis_index("col")
    row = lax.axis_index("row")
    width = query_ref.shape[1] // 8

    def features(first, count):
        blocks = [token_block(arrived_ref, first + k) for k in range(count)]
        return side_by_side(blocks, width)[:, : count * width].astype(BF16)

    own = features(col * 8, 8)
    own_four = jnp.concatenate([own] * 4, axis=0)
    across = features(row * 4, 4)
    across_four = jnp.concatenate([across] * 4, axis=0)

    low = lax.dot_general(own, down_ref[...], NN, preferred_element_type=F32)
    low_upper = low.astype(BF16)
    low_rest = (low - low_upper.astype(F32)).astype(BF16)
    query = lax.dot_general(query_ref[...], own_four, NT, preferred_element_type=F32)
    key = lax.dot_general(key_ref[...], own_four, NT, preferred_element_type=F32)
    gate = lax.dot_general(
        up_ref[...], jnp.concatenate([low_upper] * 4, axis=0), NT, preferred_element_type=F32
    ) + lax.dot_general(
        up_ref[...], jnp.concatenate([low_rest] * 4, axis=0), NT, preferred_element_type=F32
    )
    beta = lax.dot_general(beta_ref[...], own_four, NT, preferred_element_type=F32)
    lane = lanes((32, 128))
    first = jnp.where(col == 0, 1.0, 0.0)
    bias = bias_ref[...].T * first
    rate = rate_ref[...].T * first
    for ch in range(16):
        at = slice(ch * 32, ch * 32 + 32)
        misc = beta
        if 0 < ch < 8:
            misc = jnp.where(lane == 96, rate[:, ch : ch + 1], rate[:, ch + 8 : ch + 9])
        if ch == 1:
            misc = jnp.where(lane == 98, rate[:, 0:1], jnp.where(lane == 99, rate[:, 8:9], misc))
        if ch >= 8:
            misc = jnp.zeros((32, 128), F32)
        mixed_ref[at, :] = jnp.where(
            lane < 32,
            query[at],
            jnp.where(lane < 64, key[at], jnp.where(lane < 96, gate[at] + bias[:, ch : ch + 1], misc)),
        )
    value = lax.dot_general(value_ref[...], across_four, NT, preferred_element_type=F32)
    wide = lanes((256, 128))
    mixed_ref[512:768, :] = jnp.where(
        wide < 32,
        value[0:256],
        jnp.where(wide < 64, value[256:512], jnp.where(wide < 96, value[512:768], value[768:1024])),
    )
    lane8 = lanes((8, 128))
    for slot in range(32):
        sums = mixed_ref[pl.ds(heads_ref[slot], 24, stride=32), :]
        tile = jnp.where(lane8 < 96, sums[8:16], pltpu.roll(late_rest_ref[slot], 96, 1))
        pair = jnp.concatenate([sums[0:8], tile], axis=0)
        out_ref[slot, 0:16, :] = pair.astype(BF16)
        rest = left_of_both(pair)
        out_ref[slot, 16:32, :] = jnp.concatenate([rest, sums[16:24]], axis=0).astype(BF16)
    out_ref[:, 32:48, :] = late_ref[...]


def spread(array, base):
    index = jnp.broadcast_to(lanes((1, 128)) // 32 + base, array.shape)
    return jnp.take_along_axis(array, index, axis=1)


def steps_kernel(arrived_ref, packed_ref, out_ref, state_ref, turned_ref, update_ref, result_ref, scale_ref):
    clip_norm = math.sqrt(DK * DV)
    steps = 4
    lane = lanes((128, 128))
    lane1 = lanes((1, 128))
    mixed = []
    for r in range(8):
        total = None
        for c in range(4):
            peer = 4 * r + c
            rest = arrived_ref[peer, 16:32, :].astype(F32)[0:8]
            part = jnp.concatenate(joined(arrived_ref[peer, 0:16, :].astype(F32), rest), axis=0)
            total = part if total is None else total + part
        mixed.append(total)
    mixed = jnp.concatenate(mixed, axis=0)
    channel = rows_of((128, 1)) % 16
    rate = jnp.where(channel == 0, pltpu.roll(mixed, 127, 0)[:, 98:99], mixed[:, 96:97])
    rate = jnp.where(channel == 8, pltpu.roll(mixed, 7, 0)[:, 99:100], rate)
    rate = jnp.where(channel > 8, pltpu.roll(mixed, 8, 0)[:, 97:98], rate)
    soft = jnp.maximum(mixed, 0.0) + jnp.log1p(jnp.exp(-jnp.abs(mixed)))
    alpha = jnp.exp(-rate * soft)
    key_size = jnp.sum(mixed * mixed, axis=0, keepdims=True)
    inverse = 1.0 / jnp.sqrt(key_size + EPSILON)
    scaled = mixed * jnp.where(lane1 < 32, DK ** (-0.5), inverse)
    cross = jnp.sum(scaled * pltpu.roll(scaled, 96, 1), axis=0, keepdims=True)
    prepared = jnp.where(lane < 64, scaled, alpha)
    write = 1.0 / (1.0 + jnp.exp(-mixed[0:1, :]))

    row8 = rows_of((8, 128))
    lane8 = lanes((8, 128))
    where_tok = (row8 // 2) * 8 + (row8 % 2) * 4 + lane8 // 32
    write8 = jnp.take_along_axis(jnp.broadcast_to(write, (8, 128)), where_tok + 96, axis=1)
    cross8 = jnp.take_along_axis(jnp.broadcast_to(cross, (8, 128)), where_tok, axis=1)

    values = []
    for c in range(4):
        total = None
        for r in range(8):
            at = slice(r * 16, r * 16 + 16)
            peer = 4 * r + c
            rest = packed_ref[peer, 16:32, :].astype(F32)
            first, second = joined(packed_ref[peer, 0:16, :].astype(F32), rest[0:8])
            state_ref[c, at, :] = jnp.concatenate([first, second], axis=0)
            tile = arrived_ref[peer, 0:16, :].astype(F32)[8:16]
            rest = jnp.where(lane8 < 32, pltpu.roll(tile, 32, 1), rest[8:16])
            first, second = joined(arrived_ref[peer, 32:48, :].astype(F32), rest)
            state_ref[4 + c, at, :] = jnp.concatenate([first, second], axis=0)
            part = arrived_ref[peer, 16:32, :].astype(F32)[8:16]
            total = part if total is None else total + part
        values.append(total)
    turned_ref[:, 0:32] = jnp.concatenate(values, axis=0).T
    turned_ref[:, 32:128] = jnp.zeros((128, 96), F32)
    value_rows = [jnp.zeros((8, 128), F32) for _ in range(4)]
    for lo in range(4):
        for octet in range(4):
            part = turned_ref[pl.ds(octet * 32 + lo, 8, stride=4), :]
            target = lo * 32 + octet * 8
            for c in range(4):
                moved = pltpu.roll(part, (target - c * 8) % 128, 1)
                value_rows[c] = jnp.where((lane8 >= target) & (lane8 < target + 8), moved, value_rows[c])

    for hi in range(2):
        factor = None
        for t in range(steps):
            at = t * 2 + hi
            tok = t * 8 + hi * 4
            alpha_now = spread(prepared, 64 + tok)
            if factor is not None:
                alpha_now = alpha_now * factor
            key_now = spread(prepared, 32 + tok)
            query_now = spread(prepared, tok)
            write_now = write8[at : at + 1]
            cross_now = cross8[at : at + 1] * write_now
            squares = jnp.zeros((1, 128), F32)
            early = []
            for c in range(4):
                decayed = alpha_now * state_ref[hi * 4 + c]
                read = jnp.sum(key_now * decayed, axis=0, keepdims=True)
                probe = jnp.sum(query_now * decayed, axis=0, keepdims=True)
                residue = value_rows[c][at : at + 1] - read
                updated = decayed + key_now * (write_now * residue)
                state_ref[hi * 4 + c] = updated
                squares = squares + jnp.sum(updated * updated, axis=0, keepdims=True)
                update_ref[c, at : at + 1, :] = residue
                early.append(probe + cross_now * residue)
            norm = jnp.zeros((1, 128), F32)
            for lo in range(4):
                inside = lane1 // 32 == lo
                whole = jnp.sum(jnp.where(inside, squares, 0.0), axis=1, keepdims=True)
                norm = jnp.where(inside, whole, norm)
            factor = 1.0 / jnp.maximum(1.0, jnp.sqrt(norm) / clip_norm)
            scale_ref[at : at + 1, :] = factor
            for c in range(4):
                result_ref[c, at : at + 1, :] = early[c] * factor

    combined = jnp.zeros((128, 128), F32)
    for hi in range(2):
        carry = None
        for t in reversed(range(steps)):
            at = t * 2 + hi
            tok = t * 8 + hi * 4
            factor = scale_ref[at : at + 1, :]
            gain = spread(prepared, 32 + tok) * (write8[at : at + 1] * factor)
            decay = spread(prepared, 64 + tok) * factor
            if carry is not None:
                gain = gain * carry
                decay = decay * carry
            carry = decay
            combined = jnp.where(lane % 32 == at, gain, combined)
        combined = jnp.where(lane % 32 == 8 + hi, carry, combined)
    for r in range(8):
        upper = combined[16 * r : 16 * r + 8]
        lower = pltpu.roll(combined[16 * r + 8 : 16 * r + 16], 16, 1)
        both = jnp.where(lane8 % 32 < 16, upper, lower)
        for c in range(4):
            pair = jnp.concatenate([update_ref[c], both], axis=0)
            rest = jnp.concatenate([left_of_both(pair), result_ref[c]], axis=0)
            out_ref[4 * r + c, 0:16, :] = pair.astype(BF16)
            out_ref[4 * r + c, 16:32, :] = rest.astype(BF16)


def finish_kernel(
    heads_ref, packed_ref, state_ref, readout_hbm, final_hbm,
    arrived_ref, update_ref, gain_ref, readout_ref, final_ref, sems,
):
    heads = state_ref.shape[3]
    for s in range(heads):
        rest = packed_ref[s, 16:32, :].astype(F32)
        update, gain = joined(packed_ref[s, 0:16, :].astype(F32), rest[0:8])
        arrived_ref[s * 24 : s * 24 + 8, :] = update
        arrived_ref[s * 24 + 8 : s * 24 + 16, :] = gain
        arrived_ref[s * 24 + 16 : s * 24 + 24, :] = rest[8:16]
    for at in range(8):
        gain_ref[at] = arrived_ref[pl.ds(8 + at, heads, stride=24), :].T
    copies = []
    for hi in range(2):
        for t in range(4):
            update_ref[t] = arrived_ref[pl.ds(t * 2 + hi, heads, stride=24), :].T
        for lo in range(4):
            stream = hi * 4 + lo
            updates = [update_ref[t, lo * 32 : lo * 32 + 32, :] for t in range(4)]
            for i in range(16):
                i_hi, i_lo = divmod(i, 8)
                base = lo * 32 + i_hi * 16
                total = state_ref[stream, i] * gain_ref[i_lo, base + 8 + hi : base + 9 + hi, :]
                for t in range(4):
                    at = base + t * 2 + hi
                    total = total + gain_ref[i_lo, at : at + 1, :] * updates[t]
                final_ref[stream, i] = total
            copies.append(pltpu.make_async_copy(final_ref.at[stream], final_hbm.at[stream], sems.at[stream]))
            copies[-1].start()
    slot = rows_of((heads, heads))
    head = lanes((heads, heads))
    order = jnp.zeros((heads, heads), F32)
    for s in range(heads):
        order = jnp.where((slot == s) & (head == heads_ref[s]), 1.0, order)
    order = order.astype(BF16)
    for at in range(8):
        t, hi = divmod(at, 2)
        result = arrived_ref[pl.ds(16 + at, heads, stride=24), :].astype(BF16)
        turned = lax.dot_general(result, order, TN, preferred_element_type=F32).astype(BF16)
        for lo in range(4):
            readout_ref[hi * 4 + lo, t] = turned[lo * 32 : lo * 32 + 32]
    copies.append(pltpu.make_async_copy(readout_ref, readout_hbm, sems.at[8]))
    copies[-1].start()
    for copy in copies:
        copy.wait()


VMEM = pl.BlockSpec(memory_space=pltpu.VMEM)
SMEM = pl.BlockSpec(memory_space=pltpu.SMEM)
ANY = pl.BlockSpec(memory_space=pl.ANY)


def shape_of(shape, dtype):
    return jax.ShapeDtypeStruct(shape, dtype)


def on_chip(shape, dtype):
    return shape_of(shape, dtype) if INTERPRET else pltpu.VMEM(shape, dtype)


def shards(
    token_ids, slot_heads, embed_table, query_weight, key_weight, value_weight, decay_down, decay_up, decay_bias,
    decay_rate, beta_weight, init_state,
):
    groups = lax.axis_size("dp")
    state = kept(init_state)
    ids = token_ids.T
    table = embed_table.T
    picked = pl.pallas_call(
        pick_kernel,
        out_shape=on_chip((groups, 24, 128), BF16),
        in_specs=[ANY, ANY],
        out_specs=VMEM,
        scratch_shapes=[
            pltpu.VMEM((4 * token_ids.shape[0], table.shape[1]), BF16),
            pltpu.VMEM(ids.shape, jnp.int32),
            pltpu.VMEM(table.shape, BF16),
            pltpu.SemaphoreType.DMA((2,)),
        ],
        interpret=INTERPRET,
        compiler_params=pltpu.CompilerParams(vmem_limit_bytes=16 << 20),
        name="pick",
    )(far(ids), far(table))
    arrived = exchange(picked, "dp")
    early, early_rest, late, late_rest = pl.pallas_call(
        pack_state_kernel,
        out_shape=(
            on_chip((32, 16, 128), BF16),
            on_chip((32, 8, 128), F32),
            on_chip((32, 16, 128), BF16),
            on_chip((32, 8, 128), F32),
        ),
        in_specs=[VMEM],
        out_specs=(VMEM, VMEM, VMEM, VMEM),
        scratch_shapes=[pltpu.VMEM((1024, 128), F32)],
        interpret=INTERPRET,
        compiler_params=pltpu.CompilerParams(vmem_limit_bytes=16 << 20),
        name="pack_state",
    )(state)
    packed = pl.pallas_call(
        add_tokens_kernel,
        out_shape=on_chip((32, 48, 128), BF16),
        in_specs=[VMEM, VMEM, VMEM, VMEM],
        out_specs=VMEM,
        interpret=INTERPRET,
        compiler_params=pltpu.CompilerParams(vmem_limit_bytes=16 << 20),
        name="add_tokens",
    )(arrived, kept(early), kept(early_rest), kept(late_rest))
    packed = exchange(packed, BOTH)
    projected = pl.pallas_call(
        project_kernel,
        out_shape=on_chip((32, 48, 128), BF16),
        in_specs=[SMEM] + [VMEM] * 11,
        out_specs=VMEM,
        scratch_shapes=[pltpu.VMEM((768, 128), F32)],
        interpret=INTERPRET,
        compiler_params=pltpu.CompilerParams(vmem_limit_bytes=16 << 20),
        name="project",
    )(
        slot_heads,
        packed,
        kept(query_weight.transpose(1, 2, 0).reshape(512, -1)),
        kept(key_weight.transpose(1, 2, 0).reshape(512, -1)),
        kept(value_weight.transpose(1, 2, 0).reshape(1024, -1)),
        kept(decay_down),
        kept(decay_up.transpose(1, 2, 0).reshape(512, -1)),
        decay_bias,
        decay_rate,
        beta_weight.T,
        kept(late),
        kept(late_rest),
    )
    projected = exchange(projected, BOTH)
    stepped = pl.pallas_call(
        steps_kernel,
        out_shape=on_chip((32, 32, 128), BF16),
        in_specs=[VMEM, VMEM],
        out_specs=VMEM,
        scratch_shapes=[
            pltpu.VMEM((8, 128, 128), F32),
            pltpu.VMEM((128, 128), F32),
            pltpu.VMEM((4, 8, 128), F32),
            pltpu.VMEM((4, 8, 128), F32),
            pltpu.VMEM((8, 128), F32),
        ],
        interpret=INTERPRET,
        compiler_params=pltpu.CompilerParams(vmem_limit_bytes=16 << 20),
        name="steps",
    )(projected, packed)
    stepped = exchange(stepped, BOTH)
    readout, final_state = pl.pallas_call(
        finish_kernel,
        out_shape=(shape_of((8, 4, 32, 32), BF16), shape_of(init_state.shape, F32)),
        in_specs=[SMEM, VMEM, VMEM],
        out_specs=(ANY, ANY),
        scratch_shapes=[
            pltpu.VMEM((768, 128), F32),
            pltpu.VMEM((4, 128, 32), F32),
            pltpu.VMEM((8, 128, 32), F32),
            pltpu.VMEM((8, 4, 32, 32), BF16),
            pltpu.VMEM((8, 16, 32, 32), F32),
            pltpu.SemaphoreType.DMA((9,)),
        ],
        interpret=INTERPRET,
        compiler_params=pltpu.CompilerParams(vmem_limit_bytes=16 << 20),
        name="finish",
    )(slot_heads, stepped, state)
    return (readout, final_state)


def solution(mesh):
    in_specs = (
        P(),
        P(),
        P("dp", ("row", "col")),
        P("col", "row", None),
        P("col", "row", None),
        P("row", "col", None),
        P("col", None),
        P(None, "row", None),
        P("row", None),
        P("row", None),
        P("col", None),
        P("dp", "row", "col", None),
    )
    out_specs = (P("dp", None, "col", None), P("dp", "row", "col", None))
    return jax.shard_map(shards, mesh=mesh, in_specs=in_specs, out_specs=out_specs, check_vma=False)
```

```python
import math

import jax
import jax.numpy as jnp
from jax import lax
from jax.experimental import pallas as pl
from jax.experimental.pallas import tpu as pltpu
from jax.sharding import PartitionSpec as P

DK = 128
DV = 128
EPSILON = 1e-06
INTERPRET = False

F32 = jnp.float32
BF16 = jnp.bfloat16
BOTH = ("row", "col")
NT = (((1,), (1,)), ((), ()))
NN = (((1,), (0,)), ((), ()))
TN = (((0,), (0,)), ((), ()))


def lanes(shape):
    return lax.broadcasted_iota(jnp.int32, shape, len(shape) - 1)


def rows_of(shape):
    return lax.broadcasted_iota(jnp.int32, shape, len(shape) - 2)


def exchange(array, axis):
    array = lax.all_to_all(array, axis, split_axis=0, concat_axis=0, tiled=True)
    return kept(array)


def far(array):
    return array if INTERPRET else pltpu.with_memory_space_constraint(array, pltpu.HBM)


def kept(array):
    return array if INTERPRET else pltpu.with_memory_space_constraint(array, pltpu.VMEM)


def pick_kernel(ids_hbm, table_hbm, out_ref, onehot_ref, ids_ref, table_ref, sems):
    steps, streams = ids_ref.shape
    feats, vocab = table_ref.shape
    groups = out_ref.shape[0]
    ids_copy = pltpu.make_async_copy(ids_hbm, ids_ref, sems.at[0])
    table_copy = pltpu.make_async_copy(table_hbm, table_ref, sems.at[1])
    ids_copy.start()
    table_copy.start()
    ids_copy.wait()
    start = lax.axis_index("dp") * vocab
    wide = jnp.broadcast_to((ids_ref[...] - start).astype(F32)[:, None, :], (steps, 8, streams))
    columns = [wide[t].T.astype(jnp.int32)[:, 0:1] for t in range(steps)]
    width = 1024
    parts = vocab // width

    def build(part):
        across = slice(part * width, (part + 1) * width)
        for t in range(steps):
            hit = columns[t] == lanes((streams, width)) + part * width
            onehot_ref[t * streams : (t + 1) * streams, across] = jnp.where(hit, 1.0, 0.0).astype(BF16)

    ahead = 2
    for part in range(ahead):
        build(part)
    table_copy.wait()
    total = None
    for part in range(parts):
        across = slice(part * width, (part + 1) * width)
        found = lax.dot_general(onehot_ref[:, across], table_ref[:, across], NT, preferred_element_type=F32)
        total = found if total is None else total + found
        if part + ahead < parts:
            build(part + ahead)
    total = jnp.concatenate([total, jnp.zeros((total.shape[0], 128 - feats), F32)], axis=1)
    steps_rows = [total[t * streams : (t + 1) * streams] for t in range(steps)]
    lane = lanes((streams, 128))
    tail = jnp.zeros((streams, 128), F32)
    for t in range(steps):
        moved = pltpu.roll(steps_rows[t], 64 + 8 * t, 1)
        tail = jnp.where((lane >= 8 * t) & (lane < 8 * t + 8), moved, tail)
    main = [jnp.where(lane < 64, steps_rows[t], pltpu.roll(steps_rows[t + 2], 64, 1)) for t in range(2)]
    main = [part.reshape(groups, 8, 128) for part in main]
    out_ref[:, 0:16, :] = jnp.concatenate(main, axis=1).astype(BF16)
    out_ref[:, 16:24, :] = tail.reshape(groups, 8, 128).astype(BF16)


LEVELS = 10
BASE = 2 * LEVELS + 1


def rounded(array):
    return array.astype(BF16).astype(F32)


def left_over(array, upper):
    share = jnp.where(upper == 0.0, 0.0, (array - upper) / jnp.where(upper == 0.0, 1.0, upper))
    return jnp.floor(share * (256.0 * LEVELS) + 0.5)


def joined(pair, both):
    first = jnp.floor(both * (1.0 / BASE) + 0.5)
    second = both - first * BASE
    unit = 1.0 / (256.0 * LEVELS)
    return pair[0:8] * (1.0 + first * unit), pair[8:16] * (1.0 + second * unit)


def left_of_both(array):
    left = left_over(array, rounded(array))
    return left[0:8] * BASE + left[8:16]


def pack_state_kernel(state_ref, early_ref, early_rest_ref, late_ref, late_rest_ref, turned_ref):
    heads = state_ref.shape[3]
    for hi in range(2):
        for i in range(16):
            block = state_ref[hi * 4 : hi * 4 + 4, i].reshape(128, heads)
            turned_ref[pl.ds(hi * 16 + i, heads, stride=32), :] = block.T
    whole = turned_ref[...].reshape(heads, 32, 128)
    for hi, (pair_ref, rest_ref) in enumerate(((early_ref, early_rest_ref), (late_ref, late_rest_ref))):
        half = whole[:, hi * 16 : hi * 16 + 16]
        pair_ref[...] = half.astype(BF16)
        left = left_over(half, rounded(half))
        rest_ref[...] = (left[:, 0:8] * BASE + left[:, 8:16]).astype(rest_ref.dtype)


def add_tokens_kernel(arrived_ref, early_ref, early_rest_ref, late_rest_ref, out_ref):
    own = arrived_ref[0].astype(F32)
    for k in range(1, arrived_ref.shape[0]):
        own = own + arrived_ref[k].astype(F32)
    lane8 = lanes((8, 128))
    main = own[0:16].astype(BF16)
    tail = own[16:24]
    out_ref[:, 0:16, :] = early_ref[...]
    for p in range(out_ref.shape[0]):
        spare = jnp.where(lane8 < 32, tail, late_rest_ref[p])
        out_ref[p, 16:32, :] = jnp.concatenate([early_rest_ref[p], spare], axis=0).astype(BF16)
        out_ref[p, 32:48, :] = main


def token_block(arrived_ref, peer):
    main = arrived_ref[peer, 32:48, :].astype(F32)
    tail = arrived_ref[peer, 16:32, :].astype(F32)[8:16]
    lane8 = lanes((8, 128))
    turned = pltpu.roll(main, 64, 1)
    groups = []
    for k in range(4):
        base = main[8 * k : 8 * k + 8] if k < 2 else turned[8 * k - 16 : 8 * k - 8]
        moved = pltpu.roll(tail, 64 - 8 * k, 1)
        groups.append(jnp.where(lane8 < 64, base, jnp.where(lane8 < 72, moved, 0.0)))
    return jnp.concatenate(groups, axis=0)


def side_by_side(blocks, width):
    count = (len(blocks) * width + 127) // 128
    tiles = [None] * count
    lane = lanes(blocks[0].shape)
    for k, block in enumerate(blocks):
        at, shift = divmod(k * width, 128)
        rolled = pltpu.roll(block, shift, 1) if shift else block
        low = jnp.where(lane >= shift, rolled, 0.0)
        tiles[at] = low if tiles[at] is None else tiles[at] + low
        if shift + width > 128:
            tiles[at + 1] = jnp.where(lane < shift, rolled, 0.0)
    return jnp.concatenate(tiles, axis=1)


def project_kernel(
    heads_ref, arrived_ref, query_ref, key_ref, value_ref, down_ref, up_ref, bias_ref, rate_ref, beta_ref,
    late_ref, late_rest_ref, out_ref, mixed_ref,
):
    col = lax.axis_index("col")
    row = lax.axis_index("row")
    width = query_ref.shape[1] // 8

    def features(first, count):
        blocks = [token_block(arrived_ref, first + k) for k in range(count)]
        return side_by_side(blocks, width)[:, : count * width].astype(BF16)

    own = features(col * 8, 8)
    own_four = jnp.concatenate([own] * 4, axis=0)
    across = features(row * 4, 4)
    across_four = jnp.concatenate([across] * 4, axis=0)

    low = lax.dot_general(own, down_ref[...], NN, preferred_element_type=F32)
    low_upper = low.astype(BF16)
    low_rest = (low - low_upper.astype(F32)).astype(BF16)
    query = lax.dot_general(query_ref[...], own_four, NT, preferred_element_type=F32)
    key = lax.dot_general(key_ref[...], own_four, NT, preferred_element_type=F32)
    gate = lax.dot_general(
        up_ref[...], jnp.concatenate([low_upper] * 4, axis=0), NT, preferred_element_type=F32
    ) + lax.dot_general(
        up_ref[...], jnp.concatenate([low_rest] * 4, axis=0), NT, preferred_element_type=F32
    )
    beta = lax.dot_general(beta_ref[...], own_four, NT, preferred_element_type=F32)
    lane = lanes((32, 128))
    first = jnp.where(col == 0, 1.0, 0.0)
    bias = bias_ref[...].T * first
    rate = rate_ref[...].T * first
    for ch in range(16):
        at = slice(ch * 32, ch * 32 + 32)
        misc = beta
        if 0 < ch < 8:
            misc = jnp.where(lane == 96, rate[:, ch : ch + 1], rate[:, ch + 8 : ch + 9])
        if ch == 1:
            misc = jnp.where(lane == 98, rate[:, 0:1], jnp.where(lane == 99, rate[:, 8:9], misc))
        if ch >= 8:
            misc = jnp.zeros((32, 128), F32)
        mixed_ref[at, :] = jnp.where(
            lane < 32,
            query[at],
            jnp.where(lane < 64, key[at], jnp.where(lane < 96, gate[at] + bias[:, ch : ch + 1], misc)),
        )
    value = lax.dot_general(value_ref[...], across_four, NT, preferred_element_type=F32)
    wide = lanes((256, 128))
    mixed_ref[512:768, :] = jnp.where(
        wide < 32,
        value[0:256],
        jnp.where(wide < 64, value[256:512], jnp.where(wide < 96, value[512:768], value[768:1024])),
    )
    lane8 = lanes((8, 128))
    for slot in range(32):
        sums = mixed_ref[pl.ds(heads_ref[slot], 24, stride=32), :]
        tile = jnp.where(lane8 < 96, sums[8:16], pltpu.roll(late_rest_ref[slot], 96, 1))
        pair = jnp.concatenate([sums[0:8], tile], axis=0)
        out_ref[slot, 0:16, :] = pair.astype(BF16)
        rest = left_of_both(pair)
        out_ref[slot, 16:32, :] = jnp.concatenate([rest, sums[16:24]], axis=0).astype(BF16)
    out_ref[:, 32:48, :] = late_ref[...]


def spread(array, base):
    index = jnp.broadcast_to(lanes((1, 128)) // 32 + base, array.shape)
    return jnp.take_along_axis(array, index, axis=1)


def steps_kernel(arrived_ref, packed_ref, out_ref, state_ref, turned_ref, update_ref, result_ref, scale_ref):
    clip_norm = math.sqrt(DK * DV)
    steps = 4
    lane = lanes((128, 128))
    lane1 = lanes((1, 128))
    mixed = []
    for r in range(8):
        total = None
        for c in range(4):
            peer = 4 * r + c
            rest = arrived_ref[peer, 16:32, :].astype(F32)[0:8]
            part = jnp.concatenate(joined(arrived_ref[peer, 0:16, :].astype(F32), rest), axis=0)
            total = part if total is None else total + part
        mixed.append(total)
    mixed = jnp.concatenate(mixed, axis=0)
    channel = rows_of((128, 1)) % 16
    rate = jnp.where(channel == 0, pltpu.roll(mixed, 127, 0)[:, 98:99], mixed[:, 96:97])
    rate = jnp.where(channel == 8, pltpu.roll(mixed, 7, 0)[:, 99:100], rate)
    rate = jnp.where(channel > 8, pltpu.roll(mixed, 8, 0)[:, 97:98], rate)
    soft = jnp.maximum(mixed, 0.0) + jnp.log1p(jnp.exp(-jnp.abs(mixed)))
    alpha = jnp.exp(-rate * soft)
    key_size = jnp.sum(mixed * mixed, axis=0, keepdims=True)
    inverse = 1.0 / jnp.sqrt(key_size + EPSILON)
    scaled = mixed * jnp.where(lane1 < 32, DK ** (-0.5), inverse)
    cross = jnp.sum(scaled * pltpu.roll(scaled, 96, 1), axis=0, keepdims=True)
    prepared = jnp.where(lane < 64, scaled, alpha)
    write = 1.0 / (1.0 + jnp.exp(-mixed[0:1, :]))

    row8 = rows_of((8, 128))
    lane8 = lanes((8, 128))
    where_tok = (row8 // 2) * 8 + (row8 % 2) * 4 + lane8 // 32
    write8 = jnp.take_along_axis(jnp.broadcast_to(write, (8, 128)), where_tok + 96, axis=1)
    cross8 = jnp.take_along_axis(jnp.broadcast_to(cross, (8, 128)), where_tok, axis=1)

    values = []
    for c in range(4):
        total = None
        for r in range(8):
            at = slice(r * 16, r * 16 + 16)
            peer = 4 * r + c
            rest = packed_ref[peer, 16:32, :].astype(F32)
            first, second = joined(packed_ref[peer, 0:16, :].astype(F32), rest[0:8])
            state_ref[c, at, :] = jnp.concatenate([first, second], axis=0)
            tile = arrived_ref[peer, 0:16, :].astype(F32)[8:16]
            rest = jnp.where(lane8 < 32, pltpu.roll(tile, 32, 1), rest[8:16])
            first, second = joined(arrived_ref[peer, 32:48, :].astype(F32), rest)
            state_ref[4 + c, at, :] = jnp.concatenate([first, second], axis=0)
            part = arrived_ref[peer, 16:32, :].astype(F32)[8:16]
            total = part if total is None else total + part
        values.append(total)
    turned_ref[:, 0:32] = jnp.concatenate(values, axis=0).T
    turned_ref[:, 32:128] = jnp.zeros((128, 96), F32)
    value_rows = [jnp.zeros((8, 128), F32) for _ in range(4)]
    for lo in range(4):
        for octet in range(4):
            part = turned_ref[pl.ds(octet * 32 + lo, 8, stride=4), :]
            target = lo * 32 + octet * 8
            for c in range(4):
                moved = pltpu.roll(part, (target - c * 8) % 128, 1)
                value_rows[c] = jnp.where((lane8 >= target) & (lane8 < target + 8), moved, value_rows[c])

    for hi in range(2):
        factor = None
        for t in range(steps):
            at = t * 2 + hi
            tok = t * 8 + hi * 4
            alpha_now = spread(prepared, 64 + tok)
            if factor is not None:
                alpha_now = alpha_now * factor
            key_now = spread(prepared, 32 + tok)
            query_now = spread(prepared, tok)
            write_now = write8[at : at + 1]
            cross_now = cross8[at : at + 1] * write_now
            squares = jnp.zeros((1, 128), F32)
            early = []
            for c in range(4):
                decayed = alpha_now * state_ref[hi * 4 + c]
                read = jnp.sum(key_now * decayed, axis=0, keepdims=True)
                probe = jnp.sum(query_now * decayed, axis=0, keepdims=True)
                residue = value_rows[c][at : at + 1] - read
                updated = decayed + key_now * (write_now * residue)
                state_ref[hi * 4 + c] = updated
                squares = squares + jnp.sum(updated * updated, axis=0, keepdims=True)
                update_ref[c, at : at + 1, :] = residue
                early.append(probe + cross_now * residue)
            norm = jnp.zeros((1, 128), F32)
            for lo in range(4):
                inside = lane1 // 32 == lo
                whole = jnp.sum(jnp.where(inside, squares, 0.0), axis=1, keepdims=True)
                norm = jnp.where(inside, whole, norm)
            factor = 1.0 / jnp.maximum(1.0, jnp.sqrt(norm) / clip_norm)
            scale_ref[at : at + 1, :] = factor
            for c in range(4):
                result_ref[c, at : at + 1, :] = early[c] * factor

    combined = jnp.zeros((128, 128), F32)
    for hi in range(2):
        carry = None
        for t in reversed(range(steps)):
            at = t * 2 + hi
            tok = t * 8 + hi * 4
            factor = scale_ref[at : at + 1, :]
            gain = spread(prepared, 32 + tok) * (write8[at : at + 1] * factor)
            decay = spread(prepared, 64 + tok) * factor
            if carry is not None:
                gain = gain * carry
                decay = decay * carry
            carry = decay
            combined = jnp.where(lane % 32 == at, gain, combined)
        combined = jnp.where(lane % 32 == 8 + hi, carry, combined)
    for r in range(8):
        upper = combined[16 * r : 16 * r + 8]
        lower = pltpu.roll(combined[16 * r + 8 : 16 * r + 16], 16, 1)
        both = jnp.where(lane8 % 32 < 16, upper, lower)
        for c in range(4):
            pair = jnp.concatenate([update_ref[c], both], axis=0)
            rest = jnp.concatenate([left_of_both(pair), result_ref[c]], axis=0)
            out_ref[4 * r + c, 0:16, :] = pair.astype(BF16)
            out_ref[4 * r + c, 16:32, :] = rest.astype(BF16)


def finish_kernel(
    heads_ref, packed_ref, state_ref, readout_hbm, final_hbm,
    arrived_ref, update_ref, gain_ref, readout_ref, final_ref, sems,
):
    heads = state_ref.shape[3]
    for s in range(heads):
        rest = packed_ref[s, 16:32, :].astype(F32)
        update, gain = joined(packed_ref[s, 0:16, :].astype(F32), rest[0:8])
        arrived_ref[s * 24 : s * 24 + 8, :] = update
        arrived_ref[s * 24 + 8 : s * 24 + 16, :] = gain
        arrived_ref[s * 24 + 16 : s * 24 + 24, :] = rest[8:16]
    for at in range(8):
        gain_ref[at] = arrived_ref[pl.ds(8 + at, heads, stride=24), :].T
    copies = []
    for hi in range(2):
        for t in range(4):
            update_ref[t] = arrived_ref[pl.ds(t * 2 + hi, heads, stride=24), :].T
        for lo in range(4):
            stream = hi * 4 + lo
            updates = [update_ref[t, lo * 32 : lo * 32 + 32, :] for t in range(4)]
            for i in range(16):
                i_hi, i_lo = divmod(i, 8)
                base = lo * 32 + i_hi * 16
                total = state_ref[stream, i] * gain_ref[i_lo, base + 8 + hi : base + 9 + hi, :]
                for t in range(4):
                    at = base + t * 2 + hi
                    total = total + gain_ref[i_lo, at : at + 1, :] * updates[t]
                final_ref[stream, i] = total
            copies.append(pltpu.make_async_copy(final_ref.at[stream], final_hbm.at[stream], sems.at[stream]))
            copies[-1].start()
    slot = rows_of((heads, heads))
    head = lanes((heads, heads))
    order = jnp.zeros((heads, heads), F32)
    for s in range(heads):
        order = jnp.where((slot == s) & (head == heads_ref[s]), 1.0, order)
    order = order.astype(BF16)
    for at in range(8):
        t, hi = divmod(at, 2)
        result = arrived_ref[pl.ds(16 + at, heads, stride=24), :].astype(BF16)
        turned = lax.dot_general(result, order, TN, preferred_element_type=F32).astype(BF16)
        for lo in range(4):
            readout_ref[hi * 4 + lo, t] = turned[lo * 32 : lo * 32 + 32]
    copies.append(pltpu.make_async_copy(readout_ref, readout_hbm, sems.at[8]))
    copies[-1].start()
    for copy in copies:
        copy.wait()


VMEM = pl.BlockSpec(memory_space=pltpu.VMEM)
SMEM = pl.BlockSpec(memory_space=pltpu.SMEM)
ANY = pl.BlockSpec(memory_space=pl.ANY)


def shape_of(shape, dtype):
    return jax.ShapeDtypeStruct(shape, dtype)


def on_chip(shape, dtype):
    return shape_of(shape, dtype) if INTERPRET else pltpu.VMEM(shape, dtype)


def shards(
    token_ids, slot_heads, embed_table, query_weight, key_weight, value_weight, decay_down, decay_up, decay_bias,
    decay_rate, beta_weight, init_state,
):
    groups = lax.axis_size("dp")
    state = kept(init_state)
    ids = token_ids.T
    table = embed_table.T
    picked = pl.pallas_call(
        pick_kernel,
        out_shape=on_chip((groups, 24, 128), BF16),
        in_specs=[ANY, ANY],
        out_specs=VMEM,
        scratch_shapes=[
            pltpu.VMEM((4 * token_ids.shape[0], table.shape[1]), BF16),
            pltpu.VMEM(ids.shape, jnp.int32),
            pltpu.VMEM(table.shape, BF16),
            pltpu.SemaphoreType.DMA((2,)),
        ],
        interpret=INTERPRET,
        compiler_params=pltpu.CompilerParams(vmem_limit_bytes=16 << 20),
        name="pick",
    )(far(ids), far(table))
    arrived = exchange(picked, "dp")
    early, early_rest, late, late_rest = pl.pallas_call(
        pack_state_kernel,
        out_shape=(
            on_chip((32, 16, 128), BF16),
            on_chip((32, 8, 128), F32),
            on_chip((32, 16, 128), BF16),
            on_chip((32, 8, 128), F32),
        ),
        in_specs=[VMEM],
        out_specs=(VMEM, VMEM, VMEM, VMEM),
        scratch_shapes=[pltpu.VMEM((1024, 128), F32)],
        interpret=INTERPRET,
        compiler_params=pltpu.CompilerParams(vmem_limit_bytes=16 << 20),
        name="pack_state",
    )(state)
    packed = pl.pallas_call(
        add_tokens_kernel,
        out_shape=on_chip((32, 48, 128), BF16),
        in_specs=[VMEM, VMEM, VMEM, VMEM],
        out_specs=VMEM,
        interpret=INTERPRET,
        compiler_params=pltpu.CompilerParams(vmem_limit_bytes=16 << 20),
        name="add_tokens",
    )(arrived, kept(early), kept(early_rest), kept(late_rest))
    packed = exchange(packed, BOTH)
    projected = pl.pallas_call(
        project_kernel,
        out_shape=on_chip((32, 48, 128), BF16),
        in_specs=[SMEM] + [VMEM] * 11,
        out_specs=VMEM,
        scratch_shapes=[pltpu.VMEM((768, 128), F32)],
        interpret=INTERPRET,
        compiler_params=pltpu.CompilerParams(vmem_limit_bytes=16 << 20),
        name="project",
    )(
        slot_heads,
        packed,
        kept(query_weight.transpose(1, 2, 0).reshape(512, -1)),
        kept(key_weight.transpose(1, 2, 0).reshape(512, -1)),
        kept(value_weight.transpose(1, 2, 0).reshape(1024, -1)),
        kept(decay_down),
        kept(decay_up.transpose(1, 2, 0).reshape(512, -1)),
        decay_bias,
        decay_rate,
        beta_weight.T,
        kept(late),
        kept(late_rest),
    )
    projected = exchange(projected, BOTH)
    stepped = pl.pallas_call(
        steps_kernel,
        out_shape=on_chip((32, 32, 128), BF16),
        in_specs=[VMEM, VMEM],
        out_specs=VMEM,
        scratch_shapes=[
            pltpu.VMEM((8, 128, 128), F32),
            pltpu.VMEM((128, 128), F32),
            pltpu.VMEM((4, 8, 128), F32),
            pltpu.VMEM((4, 8, 128), F32),
            pltpu.VMEM((8, 128), F32),
        ],
        interpret=INTERPRET,
        compiler_params=pltpu.CompilerParams(vmem_limit_bytes=16 << 20),
        name="steps",
    )(projected, packed)
    stepped = exchange(stepped, BOTH)
    readout, final_state = pl.pallas_call(
        finish_kernel,
        out_shape=(shape_of((8, 4, 32, 32), BF16), shape_of(init_state.shape, F32)),
        in_specs=[SMEM, VMEM, VMEM],
        out_specs=(ANY, ANY),
        scratch_shapes=[
            pltpu.VMEM((768, 128), F32),
            pltpu.VMEM((4, 128, 32), F32),
            pltpu.VMEM((8, 128, 32), F32),
            pltpu.VMEM((8, 4, 32, 32), BF16),
            pltpu.VMEM((8, 16, 32, 32), F32),
            pltpu.SemaphoreType.DMA((9,)),
        ],
        interpret=INTERPRET,
        compiler_params=pltpu.CompilerParams(vmem_limit_bytes=16 << 20),
        name="finish",
    )(slot_heads, stepped, state)
    return (readout, final_state)


def solution(mesh):
    in_specs = (
        P(),
        P(),
        P("dp", ("row", "col")),
        P("col", "row", None),
        P("col", "row", None),
        P("row", "col", None),
        P("col", None),
        P(None, "row", None),
        P("row", None),
        P("row", None),
        P("col", None),
        P("dp", "row", "col", None),
    )
    out_specs = (P("dp", None, "col", None), P("dp", "row", "col", None))
    return jax.shard_map(shards, mesh=mesh, in_specs=in_specs, out_specs=out_specs, check_vma=False)
```
